32 devices in a mesh: sub: 16 (over z, x, core), rng: 2 (over y).
Axes of the slice: x: 2, y: 2, z: 4, core: 2. Of those that a mesh axis runs over, the one named last changes fastest.
Arguments:
- raw_echoes: bfloat16 [2, 4096, 4096], P(None, ('sub', 'rng')), may hold values from -6 to 6
- merge_taps: int32 [4, 2, 8, 512], replicated, may hold values from 0 to 255
- merge_weights: float32 [4, 2, 8, 512], replicated, may hold values from -2 to 2
- track_offsets: int32 [4, 16], replicated, may hold values from 0 to 63
Outputs:
- despeckled: float32 [4096, 4096], P('sub', 'rng')
The draws below stay inside these ranges and needn't reach their ends.
All inputs are finite; a program needn't handle non-finite values.
Results may differ from the reference program's by a relative error of at most 0.0045.
Values may be sent and summed in bfloat16 or wider, within the bound.
No kernel may reach another device: no remote copies, remote signals or barrier semaphores. Data moves between devices by JAX's collectives and lax.ppermute only.
A program may use at most 64 MiB of HBM per device.

```python
import math
import jax
import jax.numpy as jnp
import numpy as np
from jax import lax

FACTOR = 64
ANG = 256
TAPS = 8
MERGES = 4
SWEEPS = 8
SAMPLES = 4096
PULSES = 4096
N_SUB = 16


def plant(entries, key, smallest, largest):
    longest = entries.shape.index(max(entries.shape))
    spots = []
    for shift in (0, 1):
        where = [jax.random.randint(jax.random.fold_in(key, axis), (), 0, length) for axis, length in enumerate(entries.shape)]
        where[longest] = (where[longest] + shift) % entries.shape[longest]
        spots.append(tuple(where))
    return entries.at[spots[0]].set(smallest).at[spots[1]].set(largest)


def levels(stream_key, extent, split, least, high):
    gain, own = 1.0, jax.random.fold_in(stream_key, 6)
    for position, blocks in split:
        draws = jnp.exp(jax.random.uniform(jax.random.fold_in(own, position), (blocks,), jnp.float32, least / len(split), high / len(split)))
        gain = gain * jnp.repeat(draws, extent[position] // blocks).reshape([-1 if axis == position else 1 for axis in range(len(extent))])
    return gain


def bell_draw(stream_key, shape, width, most, pieces=(), held_as=jnp.bfloat16):
    entries = jax.random.normal(stream_key, shape, jnp.float32) * width
    if len(pieces) > 0:
        entries = levels(stream_key, shape, pieces, -0.22, 0.18) * entries
    return jnp.clip(entries, min=-most, max=most).astype(held_as)


def setup_inputs(seed: int = 0) -> dict:
    keys = jax.random.split(jax.random.key(seed), 5)
    return {
        "raw_echoes": bell_draw(keys[0], (2, PULSES, SAMPLES), 1.0, 6.0, ((1, 32),)),
        "merge_taps": plant(jax.random.randint(keys[1], (MERGES, 2, TAPS, 2 * ANG), 0, ANG), jax.random.fold_in(keys[1], 1), 0, ANG - 1).astype(jnp.int32),
        "merge_weights": bell_draw(keys[2], (MERGES, 2, TAPS, 2 * ANG), TAPS ** -0.5, 2.0, (), jnp.float32),
        "track_offsets": plant(jax.random.randint(keys[3], (MERGES, N_SUB), 0, 64), jax.random.fold_in(keys[3], 1), 0, 63).astype(jnp.int32),
    }


inv_root_two = 0.7071067811865476
diffusion_rate = 0.5
edge_scale = 2.0
phase_period = 8192

def complex_mix(real_in, imag_in, cosine_table, sine_table, form):
    highest = lax.Precision.HIGHEST
    real_out = jnp.einsum(form, real_in, cosine_table, precision=highest) + jnp.einsum(form, imag_in, sine_table, precision=highest)
    imag_out = jnp.einsum(form, imag_in, cosine_table, precision=highest) - jnp.einsum(form, real_in, sine_table, precision=highest)
    return (real_out, imag_out)

def range_transform(raw_block, factor):
    row_count = raw_block.shape[1]
    samples_all = factor * factor
    samples_in = raw_block.astype(jnp.float32).reshape(2, row_count, factor, factor)
    sample_index = jnp.arange(factor, dtype=jnp.int32)
    product = sample_index[:, None] * sample_index[None, :]
    coarse = 2.0 * math.pi / factor * (product % factor).astype(jnp.float32)
    twiddle = 2.0 * math.pi / samples_all * (product % samples_all).astype(jnp.float32)
    cosine_table = jnp.cos(coarse)
    sine_table = jnp.sin(coarse)
    first_real, first_imag = complex_mix(samples_in[0], samples_in[1], cosine_table, sine_table, 'pab,ac->pbc')
    twist_cos = jnp.cos(twiddle)
    twist_sin = jnp.sin(twiddle)
    second_real = first_real * twist_cos + first_imag * twist_sin
    second_imag = first_imag * twist_cos - first_real * twist_sin
    final_real, final_imag = complex_mix(second_real, second_imag, cosine_table, sine_table, 'pbc,bd->pdc')
    norm_scale = 1.0 / factor
    return jnp.stack([final_real, final_imag]).reshape(2, row_count, samples_all) * norm_scale

def beam_tables(angle_count, leaf_pulses):
    angle_index = jnp.arange(angle_count, dtype=jnp.int32) - angle_count // 2
    pulse_index = jnp.arange(leaf_pulses, dtype=jnp.int32)
    wrapped = angle_index[:, None] * pulse_index[None, :] % leaf_pulses
    angles_now = 2.0 * math.pi / leaf_pulses * wrapped.astype(jnp.float32)
    norm_scale = 1.0 / math.sqrt(leaf_pulses)
    return ((jnp.cos(angles_now) * norm_scale).astype(jnp.bfloat16), (jnp.sin(angles_now) * norm_scale).astype(jnp.bfloat16))

def form_leaf(compressed, cosine_table, sine_table):
    real_part = jnp.dot(cosine_table, compressed[0], preferred_element_type=jnp.float32) + jnp.dot(sine_table, compressed[1], preferred_element_type=jnp.float32)
    imag_part = jnp.dot(cosine_table, compressed[1], preferred_element_type=jnp.float32) - jnp.dot(sine_table, compressed[0], preferred_element_type=jnp.float32)
    return jnp.stack([real_part, imag_part]).astype(jnp.bfloat16)

def interp_matrix(taps_rows, weights_rows, angle_count):
    columns = jnp.arange(angle_count, dtype=jnp.int32)
    summed = jnp.zeros((taps_rows.shape[1], angle_count), jnp.float32)
    for tap_index in range(taps_rows.shape[0]):
        summed = summed + jnp.where(taps_rows[tap_index][:, None] == columns[None, :], weights_rows[tap_index][:, None], 0.0)
    return summed.astype(jnp.bfloat16)

def contribute(sector_image, matrix, offset, row_anchor, col_anchor):
    proj_real = jnp.dot(matrix, sector_image[0], preferred_element_type=jnp.float32)
    proj_imag = jnp.dot(matrix, sector_image[1], preferred_element_type=jnp.float32)
    row_index = row_anchor + jnp.arange(matrix.shape[0], dtype=jnp.int32)
    col_index = col_anchor + 1 + jnp.arange(sector_image.shape[2], dtype=jnp.int32)
    wrapped = (offset * row_index % phase_period)[:, None] * col_index[None, :] % phase_period
    motion_phase = 2.0 * math.pi / phase_period * wrapped.astype(jnp.float32)
    cosine_now = jnp.cos(motion_phase)
    sine_now = jnp.sin(motion_phase)
    return jnp.stack([proj_real * cosine_now - proj_imag * sine_now, proj_real * sine_now + proj_imag * cosine_now])

def conduct(difference):
    scaled = difference / edge_scale
    return 1.0 / (1.0 + scaled * scaled)

def diffuse(padded):
    center = padded[:, 1:-1]
    upper_diff = padded[:, 2:] - center
    lower_diff = center - padded[:, :-2]
    return center + diffusion_rate * (conduct(upper_diff) * upper_diff - conduct(lower_diff) * lower_diff)

def reference(raw_echoes, merge_taps, merge_weights, track_offsets):
    leaf_pulses = raw_echoes.shape[1] // N_SUB
    cosine_table, sine_table = beam_tables(ANG, leaf_pulses)

    def leaf_one(block_index):
        block = lax.dynamic_slice_in_dim(raw_echoes, (block_index * leaf_pulses).astype(jnp.int32), leaf_pulses, 1)
        compressed = range_transform(block, FACTOR).astype(jnp.bfloat16)
        return form_leaf(compressed, cosine_table, sine_table)
    images = lax.map(leaf_one, jnp.arange(N_SUB, dtype=jnp.int32))
    leaves = np.arange(N_SUB)
    sectors = np.zeros(N_SUB, dtype=np.int64)
    for merge_level in range(MERGES):
        partner_bit = 1 << merge_level
        sides = leaves >> merge_level & 1
        matrices = jnp.stack([interp_matrix(merge_taps[merge_level, half], merge_weights[merge_level, half], ANG) for half in range(2)])

        def part_one(items):
            sector_image, half_bit, offset, sector_now = items
            return contribute(sector_image, matrices[half_bit], offset, sector_now * (2 * ANG), jnp.int32(0))
        parts = lax.map(part_one, (images, jnp.asarray(sides, dtype=jnp.int32), track_offsets[merge_level], jnp.asarray(sectors, dtype=jnp.int32)))
        halves = parts.reshape(N_SUB, 2, 2, ANG, SAMPLES)
        own_half = halves[leaves, :, sides]
        partner_half = halves[leaves ^ partner_bit, :, sides]
        images = ((own_half + partner_half) * inv_root_two).astype(jnp.bfloat16)
        sectors = sectors * 2 + sides
    real_part = images[:, 0].astype(jnp.float32)
    imag_part = images[:, 1].astype(jnp.float32)
    intensity = jnp.sqrt(real_part * real_part + imag_part * imag_part).reshape(N_SUB * ANG, SAMPLES)
    for sweep_index in range(SWEEPS):
        padded = jnp.pad(intensity, ((0, 0), (1, 1)), mode='symmetric')
        intensity = diffuse(padded)
    return intensity
```

```python
import math

import jax
import jax.numpy as jnp
import numpy as np
from jax import lax
from jax.experimental import pallas as pl
from jax.experimental.pallas import tpu as pltpu
from jax.sharding import PartitionSpec as P

FACTOR = 64
ANG = 256
MERGES = 4
SWEEPS = 8

inv_root_two = 0.7071067811865476
phase_period = 8192

GROUP = 1 << MERGES
ROWS = 16
LANES = 128
diffusion_scale = math.sqrt(0.5)

VMEM_BYTES = 56 << 20


def bf16(table):
    return np.asarray(table, np.float32).astype(jnp.bfloat16)


def transform_tables(col_count, rng_count, norm_scale):
    index = np.arange(col_count)
    angle = 2.0 * np.pi / col_count * (np.outer(index, index) % col_count)
    cosine, sine = np.cos(angle) * norm_scale, np.sin(angle) * norm_scale
    real_rows = np.concatenate([cosine, sine], axis=1)
    imag_rows = np.concatenate([-sine, cosine], axis=1)
    swath = col_count // rng_count
    parts = [p[r * swath : (r + 1) * swath] for r in range(rng_count) for p in (real_rows, imag_rows)]
    twist = 2.0 * np.pi / (GROUP * col_count) * np.outer(np.arange(GROUP), index)
    return bf16(np.concatenate(parts)), np.stack([np.cos(twist), np.sin(twist)]).astype(np.float32)


def beam_table(leaf_pulses, rng_count):
    wrapped = np.outer(np.arange(ANG) - ANG // 2, np.arange(leaf_pulses)) % leaf_pulses
    angles = 2.0 * np.pi / leaf_pulses * wrapped
    norm_scale = 1.0 / math.sqrt(leaf_pulses)
    cosine, sine = np.cos(angles).T * norm_scale, np.sin(angles).T * norm_scale
    from_real = np.concatenate([cosine, -sine], axis=1)
    from_imag = np.concatenate([sine, cosine], axis=1)
    rows = leaf_pulses // rng_count
    parts = [f[r * rows : (r + 1) * rows] for r in range(rng_count) for f in (from_real, from_imag)]
    return bf16(np.concatenate(parts))


def turned(value, numerator, denominator):
    real, imag = value
    eighth = numerator * 8 % (8 * denominator) / denominator
    if eighth == 0:
        return real, imag
    if eighth == 2:
        return imag, -real
    if eighth == 1:
        return (real + imag) * inv_root_two, (imag - real) * inv_root_two
    if eighth == 3:
        return (imag - real) * inv_root_two, -(real + imag) * inv_root_two
    angle = 2.0 * math.pi * numerator / denominator
    c, s = math.cos(angle), math.sin(angle)
    return real * c + imag * s, imag * c - real * s


def small_transform(values):
    count = len(values)
    if count == 1:
        return values
    even, odd = small_transform(values[0::2]), small_transform(values[1::2])
    low, high = [], []
    for j in range(count // 2):
        real, imag = turned(odd[j], j, count)
        low.append((even[j][0] + real, even[j][1] + imag))
        high.append((even[j][0] - real, even[j][1] - imag))
    return low + high


def transform_kernel(raw_ref, matrix_ref, twist_ref, out_ref, stage_ref):
    col_count = raw_ref.shape[2] // GROUP
    pulses = raw_ref.shape[1]

    @pl.loop(0, pulses // ROWS)
    def _(step):
        rows = pl.ds(pl.multiple_of(step * ROWS, ROWS), ROWS)
        for lane in range(0, col_count, LANES):
            values = []
            for a in range(GROUP):
                cols = pl.ds(a * col_count + lane, LANES)
                values.append(tuple(raw_ref[part, rows, cols].astype(jnp.float32) for part in range(2)))
            for c, (real, imag) in enumerate(small_transform(values)):
                if c:
                    cos = twist_ref[0, c : c + 1, lane : lane + LANES]
                    sin = twist_ref[1, c : c + 1, lane : lane + LANES]
                    real, imag = real * cos + imag * sin, imag * cos - real * sin
                stage_ref[c, rows, lane : lane + LANES] = real.astype(jnp.bfloat16)
                stage_ref[c, rows, col_count + lane : col_count + lane + LANES] = imag.astype(jnp.bfloat16)

    pair = 2

    @pl.loop(0, GROUP // pair)
    def _(step):
        held = stage_ref[pl.ds(step * pair, pair)].reshape(pair * pulses, 2 * col_count)
        mixed = lax.dot_general(
            matrix_ref[...], held, (((1,), (1,)), ((), ())), preferred_element_type=jnp.float32
        ).astype(jnp.bfloat16)
        for j in range(pair):
            out_ref[step * pair + j] = mixed[:, j * pulses : (j + 1) * pulses]


def range_transform(raw_echoes, rng_count):
    pulses, samples = raw_echoes.shape[1:]
    col_count = samples // GROUP
    matrix, twist = transform_tables(col_count, rng_count, 1.0 / FACTOR)
    return pl.pallas_call(
        transform_kernel,
        out_shape=jax.ShapeDtypeStruct((GROUP, 2 * col_count, pulses), jnp.bfloat16),
        scratch_shapes=[pltpu.VMEM((GROUP, pulses, 2 * col_count), jnp.bfloat16)],
        compiler_params=pltpu.CompilerParams(vmem_limit_bytes=VMEM_BYTES),
        name="range_transform",
    )(raw_echoes, jnp.asarray(matrix), jnp.asarray(twist))


def unit_turn(steps):
    quarter = phase_period // 4
    turn = (steps + quarter // 2) // quarter
    x = (steps - turn * quarter).astype(jnp.float32) * (2.0 * math.pi / phase_period)
    x2 = x * x
    cos = 1.0 + x2 * (-1 / 2 + x2 * (1 / 24 + x2 * (-1 / 720 + x2 * (1 / 40320 + x2 * (-1 / 3628800)))))
    sin = x + x * (x2 * (-1 / 6 + x2 * (1 / 120 + x2 * (-1 / 5040 + x2 * (1 / 362880)))))
    odd = turn % 2 == 1
    cos, sin = jnp.where(odd, sin, cos), jnp.where(odd, cos, sin)
    cos = jnp.where((turn == 1) | (turn == 2), -cos, cos)
    sin = jnp.where((turn == 2) | (turn == 3), -sin, sin)
    return cos, sin


def tables_kernel(place_ref, offsets_ref, taps_ref, weights_ref, interp_ref, base_ref, step_ref):
    tap_count = taps_ref.shape[1]
    chunk = 64
    wide = taps_ref.shape[2]

    @pl.loop(0, taps_ref.shape[0])
    def _(matrix):
        for lane in range(0, wide, LANES):
            cols = slice(lane, lane + LANES)
            for a in range(0, ANG, chunk):
                index = lax.broadcasted_iota(jnp.int32, (chunk, LANES), 0) + a
                summed = jnp.zeros((chunk, LANES), jnp.float32)
                for t in range(tap_count):
                    taps = taps_ref[matrix, t : t + 1, cols]
                    summed = summed + jnp.where(taps == index, weights_ref[matrix, t : t + 1, cols], 0.0)
                interp_ref[matrix, a : a + chunk, cols] = summed.astype(jnp.bfloat16)

    first_bin = place_ref[0]
    first_leaf = place_ref[1]
    for level in range(MERGES):

        @pl.loop(0, GROUP)
        def _(leaf):
            sector = jnp.int32(0)
            for j in range(level):
                sector = sector * 2 + (leaf >> j & 1)
            offset = offsets_ref[level, first_leaf + leaf]
            where = level * GROUP + leaf
            for lane in range(0, wide, LANES):
                cols = slice(lane, lane + LANES)
                angle = sector * wide + lane + lax.broadcasted_iota(jnp.int32, (ROWS, LANES), 1)
                per_bin = offset * angle % phase_period
                bins = first_bin + GROUP * lax.broadcasted_iota(jnp.int32, (ROWS, LANES), 0)
                cos, sin = unit_turn(per_bin * bins % phase_period)
                base_ref[where, 0, :, cols] = cos * inv_root_two
                base_ref[where, 1, :, cols] = sin * inv_root_two
                cos, sin = unit_turn(per_bin[:8] * (GROUP * ROWS) % phase_period)
                step_ref[where, 0, :, cols] = cos
                step_ref[where, 1, :, cols] = sin


def merge_tables(merge_taps, merge_weights, track_offsets, place):
    level_halves = 2 * MERGES
    taps = merge_taps.reshape(level_halves, *merge_taps.shape[2:])
    weights = merge_weights.reshape(level_halves, *merge_taps.shape[2:])
    smem = pl.BlockSpec(memory_space=pltpu.SMEM)
    vmem = pl.BlockSpec(memory_space=pltpu.VMEM)
    wide = 2 * ANG
    return pl.pallas_call(
        tables_kernel,
        in_specs=[smem, smem, vmem, vmem],
        out_shape=(
            jax.ShapeDtypeStruct((level_halves, ANG, wide), jnp.bfloat16),
            jax.ShapeDtypeStruct((MERGES * GROUP, 2, ROWS, wide), jnp.float32),
            jax.ShapeDtypeStruct((MERGES * GROUP, 2, 8, wide), jnp.float32),
        ),
        compiler_params=pltpu.CompilerParams(vmem_limit_bytes=VMEM_BYTES),
        name="merge_tables",
    )(place, track_offsets, taps, weights)


def product(a, b):
    return a[0] * b[0] - a[1] * b[1], a[0] * b[1] + a[1] * b[0]


def merge_kernel(pulses_ref, beam_ref, interp_ref, base_ref, step_ref, out_ref, image_ref, mixed_ref):
    bins = pulses_ref.shape[2]
    parts = pulses_ref.shape[1]
    batch = 4

    @pl.loop(0, GROUP // batch)
    def _(step):
        leaves = pl.ds(step * batch, batch)
        held = jnp.concatenate(
            [pulses_ref[leaves, j].reshape(batch * bins, pulses_ref.shape[3]) for j in range(parts)], axis=1
        )
        formed = jnp.dot(held, beam_ref[...], preferred_element_type=jnp.float32).astype(jnp.bfloat16)
        for j in range(batch):
            rows = formed[j * bins : (j + 1) * bins]
            image_ref[step * batch + j, :bins] = rows[:, :ANG]
            image_ref[step * batch + j, bins:] = rows[:, ANG:]

    for level in range(MERGES):

        @pl.loop(0, GROUP // 2)
        def _(index):
            low = (index >> level << (level + 1)) | (index & ((1 << level) - 1))
            pair = (low, low + (1 << level))
            for side in range(2):
                mixed_ref[side] = jnp.dot(
                    image_ref[pair[side]], interp_ref[2 * level + side], preferred_element_type=jnp.float32
                )
            for lane in range(0, 2 * ANG, 2 * LANES):
                cols = slice(lane, lane + 2 * LANES)
                turns, steps = [], []
                for side in range(2):
                    where = level * GROUP + pair[side]
                    turns.append(tuple(base_ref[where, part, :, cols] for part in range(2)))
                    steps.append(
                        tuple(jnp.concatenate([step_ref[where, part, :, cols]] * (ROWS // 8)) for part in range(2))
                    )
                target = pair[lane // ANG]
                for row in range(0, bins, ROWS):
                    if row:
                        turns = [product(turns[side], steps[side]) for side in range(2)]
                    real, imag = 0.0, 0.0
                    for side in range(2):
                        held = tuple(
                            mixed_ref[side, part * bins + row : part * bins + row + ROWS, cols] for part in range(2)
                        )
                        r, i = product(turns[side], held)
                        real, imag = real + r, imag + i
                    if level == MERGES - 1:
                        out_ref[target, row : row + ROWS, :] = jnp.sqrt(real * real + imag * imag).astype(
                            out_ref.dtype
                        )
                    else:
                        image_ref[target, row : row + ROWS, :] = real.astype(jnp.bfloat16)
                        image_ref[target, bins + row : bins + row + ROWS, :] = imag.astype(jnp.bfloat16)


def merged_magnitude(pulses, beam, interp, base, step):
    bins = pulses.shape[2]
    return pl.pallas_call(
        merge_kernel,
        out_shape=jax.ShapeDtypeStruct((GROUP, bins, ANG), jnp.bfloat16),
        scratch_shapes=[
            pltpu.VMEM((GROUP, 2 * bins, ANG), jnp.bfloat16),
            pltpu.VMEM((2, 2 * bins, 2 * ANG), jnp.float32),
        ],
        compiler_params=pltpu.CompilerParams(vmem_limit_bytes=VMEM_BYTES),
        name="merged_magnitude",
    )(pulses, beam, interp, base, step)


def diffuse_kernel(ends_ref, cells_ref, below_ref, above_ref, out_ref, ping_ref, pong_ref):
    bins = cells_ref.shape[1]
    pitch = bins + 16
    first, last = ends_ref[0] == 1, ends_ref[1] == 1
    half = GROUP // 2

    blocks = [slice(h * LANES, (h + 1) * LANES) for h in range(ANG // LANES)]
    for h, cols in enumerate(blocks):
        for c in range(GROUP):
            cells = cells_ref[c, :, cols].astype(jnp.float32)
            ping_ref[h, c * pitch + 8 : c * pitch + 8 + bins] = cells * diffusion_scale
        for j in range(half):
            down, up = half + j, j
            own = ping_ref[h, (GROUP - 1 - down) * pitch + 8 : (GROUP - 1 - down) * pitch + 9]
            sent = below_ref[j : j + 1, cols].astype(jnp.float32) * diffusion_scale
            ping_ref[h, down * pitch + 7 : down * pitch + 8] = jnp.where(first, own, sent)
            own = ping_ref[h, (GROUP - 1 - up) * pitch + 7 + bins : (GROUP - 1 - up) * pitch + 8 + bins]
            sent = above_ref[j : j + 1, cols].astype(jnp.float32) * diffusion_scale
            ping_ref[h, up * pitch + 8 + bins : up * pitch + 9 + bins] = jnp.where(last, own, sent)

    def flux(upper, lower):
        difference = upper - lower
        return difference / (2.0 + difference * difference)

    sublane = lax.broadcasted_iota(jnp.int32, (8, LANES), 0)

    def tile(source, target, h, row, begin, end):
        def cells(c, shift=0):
            return source[h, pl.ds(c * pitch + row + shift, 8)]

        def before():
            near, far = pltpu.roll(cells(GROUP - 1), 1, 0), pltpu.roll(cells(GROUP - 1, -8), 1, 0)
            return jnp.where(sublane == 0, far, near)

        def after():
            near, far = pltpu.roll(cells(0), 7, 0), pltpu.roll(cells(0, 8), 7, 0)
            return jnp.where(sublane == 7, far, near)

        here = cells(begin)
        flow = flux(here, before()) if begin == 0 else None
        for c in range(begin, end):
            if c < end - 1:
                there = cells(c + 1)
            elif end == GROUP:
                there = after()
            else:
                there = None
            ahead = flux(there, here) if there is not None else None
            value = here
            if ahead is not None:
                value = value + ahead
            if flow is not None:
                value = value - flow
            target[h, pl.ds(c * pitch + row, 8)] = value
            here, flow = there, ahead

    def sweep(source, target):
        for h in range(len(blocks)):
            tile(source, target, h, 0, half, GROUP)
            tile(source, target, h, 8 + bins, 0, half)

        @pl.loop(0, bins // 8)
        def _(step):
            for h in range(len(blocks)):
                tile(source, target, h, pl.multiple_of(8 + 8 * step, 8), 0, GROUP)

    @pl.loop(0, SWEEPS // 2)
    def _(step):
        sweep(ping_ref, pong_ref)
        sweep(pong_ref, ping_ref)

    rows = LANES // GROUP

    @pl.loop(0, bins // rows)
    def _(step):
        for h, cols in enumerate(blocks):
            held = jnp.concatenate(
                [ping_ref[h, pl.ds(8 + step * rows + d, GROUP, stride=pitch)] for d in range(rows)]
            )
            out_ref[cols, pl.ds(pl.multiple_of(step * LANES, LANES), LANES)] = held.T * (1.0 / diffusion_scale)


def despeckle(cells, below, above, ends):
    bins = cells.shape[1]
    smem = pl.BlockSpec(memory_space=pltpu.SMEM)
    vmem = pl.BlockSpec(memory_space=pltpu.VMEM)
    return pl.pallas_call(
        diffuse_kernel,
        in_specs=[smem, vmem, vmem, vmem],
        out_shape=jax.ShapeDtypeStruct((ANG, GROUP * bins), jnp.float32),
        scratch_shapes=[pltpu.VMEM((ANG // LANES, GROUP * (bins + 16), LANES), jnp.float32)] * 2,
        compiler_params=pltpu.CompilerParams(vmem_limit_bytes=VMEM_BYTES),
        name="despeckle",
    )(ends, cells, below, above)


def per_device(raw_echoes, merge_taps, merge_weights, track_offsets):
    sub_count, rng_count = lax.axis_size("sub"), lax.axis_size("rng")
    leaf, position = lax.axis_index("sub"), lax.axis_index("rng")
    pulses, samples = raw_echoes.shape[1:]
    bins = samples // (GROUP * rng_count)
    groups = [[g * GROUP + i for i in range(GROUP)] for g in range(sub_count // GROUP)]
    groups = groups if len(groups) > 1 else None

    compressed = range_transform(raw_echoes, rng_count)
    place = jnp.stack([leaf % GROUP + 1 + position * (bins * GROUP), leaf // GROUP * GROUP]).astype(jnp.int32)
    tables = merge_tables(merge_taps, merge_weights, track_offsets, place)
    if groups is None:
        blocks = compressed.reshape(GROUP * rng_count, 2 * bins, pulses)
        regrouped = lax.all_to_all(blocks, ("sub", "rng"), split_axis=0, concat_axis=0, tiled=True)
    else:
        blocks = compressed.reshape(GROUP, rng_count, 2 * bins, pulses)
        blocks = lax.all_to_all(blocks, "rng", split_axis=1, concat_axis=1, tiled=True)
        regrouped = lax.all_to_all(
            blocks, "sub", split_axis=0, concat_axis=0, tiled=True, axis_index_groups=groups
        )
    regrouped = regrouped.reshape(GROUP, rng_count * 2, bins, pulses)
    beam = jnp.asarray(beam_table(pulses * rng_count, rng_count))
    magnitude = merged_magnitude(regrouped, beam, *tables)
    cells = lax.all_to_all(
        magnitude, "sub", split_axis=0, concat_axis=0, tiled=True, axis_index_groups=groups
    )
    half = GROUP // 2
    ends = rng_count - 1
    below = lax.ppermute(cells[half:, -1], "rng", [(i, i + 1) for i in range(ends)])
    above = lax.ppermute(cells[:half, 0], "rng", [(i + 1, i) for i in range(ends)])
    flags = jnp.stack([position == 0, position == rng_count - 1]).astype(jnp.int32)
    return despeckle(cells, below, above, flags)


def solution(mesh):
    in_specs = (P(None, ("sub", "rng"), None), P(), P(), P())
    out_specs = P("sub", "rng")
    return jax.shard_map(
        per_device, mesh=mesh, in_specs=in_specs, out_specs=out_specs, check_vma=False
    )
```

```python
import functools
import math

import jax
import jax.numpy as jnp
import numpy as np
from jax import lax
from jax.experimental import pallas as pl
from jax.experimental.pallas import tpu as pltpu
from jax.sharding import PartitionSpec as P

FACTOR = 64
ANG = 256
MERGES = 4
SWEEPS = 8

inv_root_two = 0.7071067811865476
phase_period = 8192

GROUP = 1 << MERGES
ROWS = 16
LANES = 128
diffusion_scale = math.sqrt(0.5)

VMEM_BYTES = 56 << 20

ANY = pl.BlockSpec(memory_space=pl.ANY)
SMEM = pl.BlockSpec(memory_space=pltpu.SMEM)
VMEM = pl.BlockSpec(memory_space=pltpu.VMEM)


def bf16(table):
    return np.asarray(table, np.float32).astype(jnp.bfloat16)


def chunked(bins):
    quarter = bins // 4
    if quarter % ROWS:
        return (((0, bins),),)
    return ((0, quarter), (3 * quarter, quarter)), ((quarter, 2 * quarter),)


def length(segments):
    return sum(count for _, count in segments)


def transform_tables(col_count, rng_count, norm_scale):
    index = np.arange(col_count)
    angle = 2.0 * np.pi / col_count * (np.outer(index, index) % col_count)
    cosine, sine = np.cos(angle) * norm_scale, np.sin(angle) * norm_scale
    real_rows = np.concatenate([cosine, sine], axis=1)
    imag_rows = np.concatenate([-sine, cosine], axis=1)
    swath = col_count // rng_count
    parts = [
        part[r * swath + start : r * swath + start + count]
        for segments in chunked(swath)
        for r in range(rng_count)
        for part in (real_rows, imag_rows)
        for start, count in segments
    ]
    twist = 2.0 * np.pi / (GROUP * col_count) * np.outer(np.arange(GROUP), index)
    return bf16(np.concatenate(parts)), np.stack([np.cos(twist), np.sin(twist)]).astype(np.float32)


def beam_table(leaf_pulses, rng_count):
    wrapped = np.outer(np.arange(ANG) - ANG // 2, np.arange(leaf_pulses)) % leaf_pulses
    angles = 2.0 * np.pi / leaf_pulses * wrapped
    norm_scale = 1.0 / math.sqrt(leaf_pulses)
    cosine, sine = np.cos(angles).T * norm_scale, np.sin(angles).T * norm_scale
    from_real = np.concatenate([cosine, -sine], axis=1)
    from_imag = np.concatenate([sine, cosine], axis=1)
    rows = leaf_pulses // rng_count
    parts = [f[r * rows : (r + 1) * rows] for r in range(rng_count) for f in (from_real, from_imag)]
    return bf16(np.concatenate(parts))


def turned(value, numerator, denominator):
    real, imag = value
    eighth = numerator * 8 % (8 * denominator) / denominator
    if eighth == 0:
        return real, imag
    if eighth == 2:
        return imag, -real
    if eighth == 1:
        return (real + imag) * inv_root_two, (imag - real) * inv_root_two
    if eighth == 3:
        return (imag - real) * inv_root_two, -(real + imag) * inv_root_two
    angle = 2.0 * math.pi * numerator / denominator
    c, s = math.cos(angle), math.sin(angle)
    return real * c + imag * s, imag * c - real * s


def small_transform(values):
    count = len(values)
    if count == 1:
        return values
    even, odd = small_transform(values[0::2]), small_transform(values[1::2])
    low, high = [], []
    for j in range(count // 2):
        real, imag = turned(odd[j], j, count)
        low.append((even[j][0] + real, even[j][1] + imag))
        high.append((even[j][0] - real, even[j][1] - imag))
    return low + high


def transform_kernel(raw_hbm, matrix_hbm, twist_ref, *refs):
    count = (len(refs) - 6) // 2
    out_hbms, refs = refs[:count], refs[count:]
    raw_ref, matrix_ref, stage_ref, *out_refs = refs[: 3 + count]
    raw_sems, matrix_sem, out_sems = refs[3 + count :]
    col_count = raw_ref.shape[2] // GROUP
    pulses = raw_ref.shape[1]
    blocks = raw_sems.shape[0]
    block = pulses // blocks
    pair = 2

    def fetch(i):
        rows = pl.ds(pl.multiple_of(i * block, block), block)
        return pltpu.make_async_copy(raw_hbm.at[:, rows], raw_ref.at[:, rows], raw_sems.at[i])

    def send(k, step):
        here = pl.ds(step * pair, pair)
        return pltpu.make_async_copy(out_refs[k].at[here], out_hbms[k].at[here], out_sems.at[k, step])

    matrix_copy = pltpu.make_async_copy(matrix_hbm, matrix_ref, matrix_sem)
    for i in range(blocks):
        fetch(i).start()
    matrix_copy.start()

    @pl.loop(0, blocks)
    def _(i):
        fetch(i).wait()

        @pl.loop(0, block // ROWS)
        def _(step):
            rows = pl.ds(pl.multiple_of(i * block + step * ROWS, ROWS), ROWS)
            for lane in range(0, col_count, LANES):
                values = []
                for a in range(GROUP):
                    cols = pl.ds(a * col_count + lane, LANES)
                    values.append(tuple(raw_ref[part, rows, cols].astype(jnp.float32) for part in range(2)))
                for c, (real, imag) in enumerate(small_transform(values)):
                    if c:
                        cos = twist_ref[0, c : c + 1, lane : lane + LANES]
                        sin = twist_ref[1, c : c + 1, lane : lane + LANES]
                        real, imag = real * cos + imag * sin, imag * cos - real * sin
                    stage_ref[c, rows, lane : lane + LANES] = real.astype(jnp.bfloat16)
                    stage_ref[c, rows, col_count + lane : col_count + lane + LANES] = imag.astype(jnp.bfloat16)

    matrix_copy.wait()

    @pl.loop(0, GROUP // pair)
    def _(step):
        held = stage_ref[pl.ds(step * pair, pair)].reshape(pair * pulses, 2 * col_count)
        mixed = lax.dot_general(
            matrix_ref[...], held, (((1,), (1,)), ((), ())), preferred_element_type=jnp.float32
        ).astype(jnp.bfloat16)
        begin = 0
        for k, out_ref in enumerate(out_refs):
            end = begin + out_ref.shape[1]
            for j in range(pair):
                out_ref[step * pair + j] = mixed[begin:end, j * pulses : (j + 1) * pulses]
            begin = end
            send(k, step).start()

    for k in range(count):
        for step in range(GROUP // pair):
            send(k, step).wait()


def range_transform(raw_echoes, rng_count):
    pulses, samples = raw_echoes.shape[1:]
    col_count = samples // GROUP
    matrix, twist = transform_tables(col_count, rng_count, 1.0 / FACTOR)
    outputs = [(GROUP, rng_count * 2 * length(segments), pulses) for segments in chunked(col_count // rng_count)]
    return pl.pallas_call(
        transform_kernel,
        in_specs=[ANY, ANY, VMEM],
        out_specs=(ANY,) * len(outputs),
        out_shape=tuple(jax.ShapeDtypeStruct(shape, jnp.bfloat16) for shape in outputs),
        scratch_shapes=[
            pltpu.VMEM(raw_echoes.shape, jnp.bfloat16),
            pltpu.VMEM(matrix.shape, jnp.bfloat16),
            pltpu.VMEM((GROUP, pulses, 2 * col_count), jnp.bfloat16),
            *[pltpu.VMEM(shape, jnp.bfloat16) for shape in outputs],
            pltpu.SemaphoreType.DMA((pulses // (2 * ROWS),)),
            pltpu.SemaphoreType.DMA,
            pltpu.SemaphoreType.DMA((len(outputs), GROUP // 2)),
        ],
        compiler_params=pltpu.CompilerParams(vmem_limit_bytes=VMEM_BYTES),
        name="range_transform",
    )(raw_echoes, jnp.asarray(matrix), jnp.asarray(twist))


def unit_turn(steps):
    quarter = phase_period // 4
    turn = (steps + quarter // 2) // quarter
    x = (steps - turn * quarter).astype(jnp.float32) * (2.0 * math.pi / phase_period)
    x2 = x * x
    cos = 1.0 + x2 * (-1 / 2 + x2 * (1 / 24 + x2 * (-1 / 720 + x2 * (1 / 40320 + x2 * (-1 / 3628800)))))
    sin = x + x * (x2 * (-1 / 6 + x2 * (1 / 120 + x2 * (-1 / 5040 + x2 * (1 / 362880)))))
    odd = turn % 2 == 1
    cos, sin = jnp.where(odd, sin, cos), jnp.where(odd, cos, sin)
    cos = jnp.where((turn == 1) | (turn == 2), -cos, cos)
    sin = jnp.where((turn == 2) | (turn == 3), -sin, sin)
    return cos, sin


def tables_kernel(place_ref, offsets_ref, taps_ref, weights_ref, interp_ref, base_ref, step_ref):
    tap_count = taps_ref.shape[1]
    chunk = 64
    wide = taps_ref.shape[2]

    @pl.loop(0, taps_ref.shape[0])
    def _(matrix):
        for lane in range(0, wide, LANES):
            cols = slice(lane, lane + LANES)
            for a in range(0, ANG, chunk):
                index = lax.broadcasted_iota(jnp.int32, (chunk, LANES), 0) + a
                summed = jnp.zeros((chunk, LANES), jnp.float32)
                for t in range(tap_count):
                    taps = taps_ref[matrix, t : t + 1, cols]
                    summed = summed + jnp.where(taps == index, weights_ref[matrix, t : t + 1, cols], 0.0)
                interp_ref[matrix, a : a + chunk, cols] = summed.astype(jnp.bfloat16)

    first_bin = place_ref[0]
    first_leaf = place_ref[1]
    for level in range(MERGES):

        @pl.loop(0, GROUP)
        def _(leaf):
            sector = jnp.int32(0)
            for j in range(level):
                sector = sector * 2 + (leaf >> j & 1)
            offset = offsets_ref[level, first_leaf + leaf]
            where = level * GROUP + leaf
            for lane in range(0, wide, LANES):
                cols = slice(lane, lane + LANES)
                angle = sector * wide + lane + lax.broadcasted_iota(jnp.int32, (8, LANES), 1)
                per_bin = offset * angle % phase_period
                bins = first_bin + GROUP * lax.broadcasted_iota(jnp.int32, (8, LANES), 0)
                cos, sin = unit_turn(per_bin * bins % phase_period)
                base_ref[where, 0, :, cols] = cos * inv_root_two
                base_ref[where, 1, :, cols] = sin * inv_root_two
                cos, sin = unit_turn(per_bin[:1] * (GROUP * 8) % phase_period)
                step_ref[where, 0:1, cols] = cos
                step_ref[where, 1:2, cols] = sin


def merge_tables(merge_taps, merge_weights, track_offsets, place):
    level_halves = 2 * MERGES
    taps = merge_taps.reshape(level_halves, *merge_taps.shape[2:])
    weights = merge_weights.reshape(level_halves, *merge_taps.shape[2:])
    wide = 2 * ANG
    return pl.pallas_call(
        tables_kernel,
        in_specs=[SMEM, SMEM, VMEM, VMEM],
        out_shape=(
            jax.ShapeDtypeStruct((level_halves, ANG, wide), jnp.bfloat16),
            jax.ShapeDtypeStruct((MERGES * GROUP, 2, 8, wide), jnp.float32),
            jax.ShapeDtypeStruct((MERGES * GROUP, 2, wide), jnp.float32),
        ),
        compiler_params=pltpu.CompilerParams(vmem_limit_bytes=VMEM_BYTES),
        name="merge_tables",
    )(place, track_offsets, taps, weights)


def product(a, b):
    return a[0] * b[0] - a[1] * b[1], a[0] * b[1] + a[1] * b[0]


def power(a, count):
    if count == 1:
        return a
    half = power(a, count // 2)
    whole = product(half, half)
    return product(whole, a) if count % 2 else whole


def merge_kernel(segments, pulses_hbm, beam_hbm, interp_hbm, base_hbm, step_hbm, out_hbm, *refs):
    pulses_ref, beam_ref, interp_ref, base_ref, step_ref, out_ref, image_ref, mixed_ref = refs[:8]
    pulse_sems, whole_sems, level_sems, out_sems = refs[8:]
    bins = pulses_ref.shape[2]
    parts = pulses_ref.shape[1]
    batch = 4

    def copy(source, target, here, sem):
        return pltpu.make_async_copy(source.at[here], target.at[here], sem)

    def pulses_copy(i):
        return copy(pulses_hbm, pulses_ref, pl.ds(i * batch, batch), pulse_sems.at[i])

    def level_copies(level):
        return (
            copy(interp_hbm, interp_ref, pl.ds(2 * level, 2), level_sems.at[level, 0]),
            copy(base_hbm, base_ref, pl.ds(level * GROUP, GROUP), level_sems.at[level, 1]),
        )

    def out_copy(leaf):
        return copy(out_ref, out_hbm, pl.ds(leaf, 1), out_sems.at[leaf])

    beam_copy = pltpu.make_async_copy(beam_hbm, beam_ref, whole_sems.at[0])
    step_copy = pltpu.make_async_copy(step_hbm, step_ref, whole_sems.at[1])
    beam_copy.start()
    for i in range(GROUP // batch):
        pulses_copy(i).start()
    step_copy.start()
    for level in range(MERGES):
        for item in level_copies(level):
            item.start()
    beam_copy.wait()

    @pl.loop(0, GROUP // batch)
    def _(step):
        pulses_copy(step).wait()
        leaves = pl.ds(step * batch, batch)
        held = jnp.concatenate(
            [pulses_ref[leaves, j].reshape(batch * bins, pulses_ref.shape[3]) for j in range(parts)], axis=1
        )
        formed = jnp.dot(held, beam_ref[...], preferred_element_type=jnp.float32).astype(jnp.bfloat16)
        for j in range(batch):
            rows = formed[j * bins : (j + 1) * bins]
            image_ref[step * batch + j, :bins] = rows[:, :ANG]
            image_ref[step * batch + j, bins:] = rows[:, ANG:]

    step_copy.wait()
    for level in range(MERGES):
        for item in level_copies(level):
            item.wait()

        def lower(index):
            return (index >> level << (level + 1)) | (index & ((1 << level) - 1))

        @pl.loop(0, GROUP // 2 // batch)
        def _(step):
            for side in range(2):
                leaves = [lower(step * batch + j) + (side << level) for j in range(batch)]
                held = jnp.concatenate([image_ref[leaf] for leaf in leaves])
                mixed = jnp.dot(held, interp_ref[2 * level + side], preferred_element_type=jnp.float32)
                for j in range(batch):
                    mixed_ref[side, step * batch + j] = mixed[j * 2 * bins : (j + 1) * 2 * bins]

        @pl.loop(0, GROUP // 2)
        def _(index):
            low = lower(index)
            pair = (low, low + (1 << level))
            for lane in range(0, 2 * ANG, 2 * LANES):
                cols = slice(lane, lane + 2 * LANES)
                turns, steps = [], []
                for side in range(2):
                    where = level * GROUP + pair[side]
                    base = tuple(base_ref[where, part, :, cols] for part in range(2))
                    step = tuple(step_ref[where, part : part + 1, cols] for part in range(2))
                    later = product(base, step)
                    turns.append(tuple(jnp.concatenate([base[part], later[part]]) for part in range(2)))
                    steps.append(product(step, step))
                target = pair[lane // ANG]
                place = 0
                spots = [start + i for start, count in segments for i in range(0, count, ROWS)]
                for row, spot in zip(range(0, bins, ROWS), spots):
                    if spot != place:
                        jumps = [power(steps[side], (spot - place) // ROWS) for side in range(2)]
                        turns = [product(turns[side], jumps[side]) for side in range(2)]
                        place = spot
                    real, imag = 0.0, 0.0
                    for side in range(2):
                        held = tuple(
                            mixed_ref[side, index, part * bins + row : part * bins + row + ROWS, cols]
                            for part in range(2)
                        )
                        r, i = product(turns[side], held)
                        real, imag = real + r, imag + i
                    if level == MERGES - 1:
                        out_ref[target, row : row + ROWS, :] = jnp.sqrt(real * real + imag * imag).astype(
                            out_ref.dtype
                        )
                    else:
                        image_ref[target, row : row + ROWS, :] = real.astype(jnp.bfloat16)
                        image_ref[target, bins + row : bins + row + ROWS, :] = imag.astype(jnp.bfloat16)
            if level == MERGES - 1:
                for leaf in pair:
                    out_copy(leaf).start()

    for leaf in range(GROUP):
        out_copy(leaf).wait()


def merged_magnitude(segments, pulses, beam, interp, base, step):
    bins = pulses.shape[2]
    inputs = (pulses, beam, interp, base, step)
    return pl.pallas_call(
        functools.partial(merge_kernel, segments),
        in_specs=[ANY] * len(inputs),
        out_specs=ANY,
        out_shape=jax.ShapeDtypeStruct((GROUP, bins, ANG), jnp.bfloat16),
        scratch_shapes=[
            *[pltpu.VMEM(array.shape, array.dtype) for array in inputs],
            pltpu.VMEM((GROUP, bins, ANG), jnp.bfloat16),
            pltpu.VMEM((GROUP, 2 * bins, ANG), jnp.bfloat16),
            pltpu.VMEM((2, GROUP // 2, 2 * bins, 2 * ANG), jnp.float32),
            pltpu.SemaphoreType.DMA((GROUP // 4,)),
            pltpu.SemaphoreType.DMA((2,)),
            pltpu.SemaphoreType.DMA((MERGES, 2)),
            pltpu.SemaphoreType.DMA((GROUP,)),
        ],
        compiler_params=pltpu.CompilerParams(vmem_limit_bytes=VMEM_BYTES),
        name="merged_magnitude",
    )(*inputs)


def diffuse_kernel(chunks, ends_ref, below_ref, above_ref, *refs):
    count = len(chunks)
    cells_hbms, out_hbm, cells_refs = refs[:count], refs[count], refs[count + 1 : 2 * count + 1]
    out_ref, ping_ref, pong_ref, cells_sems, out_sems = refs[2 * count + 1 :]
    copies = [
        pltpu.make_async_copy(cells_hbms[k], cells_refs[k], cells_sems.at[k]) for k in range(count)
    ]
    for item in copies:
        item.start()
    bins = sum(length(segments) for segments in chunks)
    pitch = bins + 16
    first, last = ends_ref[0] == 1, ends_ref[1] == 1
    half = GROUP // 2

    blocks = [slice(h * LANES, (h + 1) * LANES) for h in range(ANG // LANES)]
    for segments, cells_ref, item in zip(chunks, cells_refs, copies):
        item.wait()
        for h, cols in enumerate(blocks):
            for c in range(GROUP):
                row = 0
                for start, length_here in segments:
                    cells = cells_ref[c, row : row + length_here, cols].astype(jnp.float32)
                    ping_ref[h, pl.ds(c * pitch + 8 + start, length_here)] = cells * diffusion_scale
                    row += length_here
    for h, cols in enumerate(blocks):
        for j in range(half):
            down, up = half + j, j
            own = ping_ref[h, (GROUP - 1 - down) * pitch + 8 : (GROUP - 1 - down) * pitch + 9]
            sent = below_ref[j : j + 1, cols].astype(jnp.float32) * diffusion_scale
            ping_ref[h, down * pitch + 7 : down * pitch + 8] = jnp.where(first, own, sent)
            own = ping_ref[h, (GROUP - 1 - up) * pitch + 7 + bins : (GROUP - 1 - up) * pitch + 8 + bins]
            sent = above_ref[j : j + 1, cols].astype(jnp.float32) * diffusion_scale
            ping_ref[h, up * pitch + 8 + bins : up * pitch + 9 + bins] = jnp.where(last, own, sent)

    def flux(upper, lower):
        difference = upper - lower
        return difference / (2.0 + difference * difference)

    sublane = lax.broadcasted_iota(jnp.int32, (8, LANES), 0)

    def tile(source, target, h, row, begin, end):
        def cells(c, shift=0):
            return source[h, pl.ds(c * pitch + row + shift, 8)]

        def before():
            near, far = pltpu.roll(cells(GROUP - 1), 1, 0), pltpu.roll(cells(GROUP - 1, -8), 1, 0)
            return jnp.where(sublane == 0, far, near)

        def after():
            near, far = pltpu.roll(cells(0), 7, 0), pltpu.roll(cells(0, 8), 7, 0)
            return jnp.where(sublane == 7, far, near)

        here = cells(begin)
        flow = flux(here, before()) if begin == 0 else None
        for c in range(begin, end):
            if c < end - 1:
                there = cells(c + 1)
            elif end == GROUP:
                there = after()
            else:
                there = None
            ahead = flux(there, here) if there is not None else None
            value = here
            if ahead is not None:
                value = value + ahead
            if flow is not None:
                value = value - flow
            target[h, pl.ds(c * pitch + row, 8)] = value
            here, flow = there, ahead

    def sweep(source, target):
        for h in range(len(blocks)):
            tile(source, target, h, 0, half, GROUP)
            tile(source, target, h, 8 + bins, 0, half)

        @pl.loop(0, bins // 8)
        def _(step):
            for h in range(len(blocks)):
                tile(source, target, h, pl.multiple_of(8 + 8 * step, 8), 0, GROUP)

    @pl.loop(0, SWEEPS // 2)
    def _(step):
        sweep(ping_ref, pong_ref)
        sweep(pong_ref, ping_ref)

    rows = LANES // GROUP

    def out_copy(step):
        cols = pl.ds(pl.multiple_of(step * LANES, LANES), LANES)
        return pltpu.make_async_copy(out_ref.at[:, cols], out_hbm.at[:, cols], out_sems.at[step])

    @pl.loop(0, bins // rows)
    def _(step):
        for h, cols in enumerate(blocks):
            held = jnp.concatenate(
                [ping_ref[h, pl.ds(8 + step * rows + d, GROUP, stride=pitch)] for d in range(rows)]
            )
            out_ref[cols, pl.ds(pl.multiple_of(step * LANES, LANES), LANES)] = held.T * (1.0 / diffusion_scale)
        out_copy(step).start()

    for step in range(bins // rows):
        out_copy(step).wait()


def despeckle(chunks, cells, below, above, ends):
    bins = sum(part.shape[1] for part in cells)
    shape = (ANG, GROUP * bins)
    return pl.pallas_call(
        functools.partial(diffuse_kernel, chunks),
        in_specs=[SMEM, VMEM, VMEM] + [ANY] * len(cells),
        out_specs=ANY,
        out_shape=jax.ShapeDtypeStruct(shape, jnp.float32),
        scratch_shapes=[
            *[pltpu.VMEM(part.shape, part.dtype) for part in cells],
            pltpu.VMEM(shape, jnp.float32),
            *[pltpu.VMEM((ANG // LANES, GROUP * (bins + 16), LANES), jnp.float32)] * 2,
            pltpu.SemaphoreType.DMA((len(cells),)),
            pltpu.SemaphoreType.DMA((GROUP * bins // LANES,)),
        ],
        compiler_params=pltpu.CompilerParams(vmem_limit_bytes=VMEM_BYTES),
        name="despeckle",
    )(ends, below, above, *cells)


def per_device(raw_echoes, merge_taps, merge_weights, track_offsets):
    sub_count, rng_count = lax.axis_size("sub"), lax.axis_size("rng")
    leaf, position = lax.axis_index("sub"), lax.axis_index("rng")
    pulses, samples = raw_echoes.shape[1:]
    bins = samples // (GROUP * rng_count)
    groups = [[g * GROUP + i for i in range(GROUP)] for g in range(sub_count // GROUP)]
    groups = groups if len(groups) > 1 else None

    chunks = chunked(bins)

    def regroup(block, count):
        if groups is None:
            block = block.reshape(GROUP * rng_count, 2 * count, pulses)
            block = lax.all_to_all(block, ("sub", "rng"), split_axis=0, concat_axis=0, tiled=True)
        else:
            block = block.reshape(GROUP, rng_count, 2 * count, pulses)
            block = lax.all_to_all(block, "rng", split_axis=1, concat_axis=1, tiled=True)
            block = lax.all_to_all(
                block, "sub", split_axis=0, concat_axis=0, tiled=True, axis_index_groups=groups
            )
        return block.reshape(GROUP, rng_count * 2, count, pulses)

    compressed = range_transform(raw_echoes, rng_count)
    place = jnp.stack([leaf % GROUP + 1 + position * (bins * GROUP), leaf // GROUP * GROUP]).astype(jnp.int32)
    tables = merge_tables(merge_taps, merge_weights, track_offsets, place)
    regrouped = []
    for block, segments in zip(compressed, chunks):
        if regrouped:
            block, tables, regrouped[-1] = lax.optimization_barrier((block, tables, regrouped[-1]))
        regrouped.append(regroup(block, length(segments)))
    beam = jnp.asarray(beam_table(pulses * rng_count, rng_count))
    cells = []
    for segments, block in zip(chunks, regrouped):
        magnitude = merged_magnitude(segments, block, beam, *tables)
        cells.append(
            lax.all_to_all(magnitude, "sub", split_axis=0, concat_axis=0, tiled=True, axis_index_groups=groups)
        )
    half = GROUP // 2
    head, tail = cells[0][:half, 0], cells[0][half:, -1]
    if rng_count == 2:
        below = above = lax.ppermute(jnp.where(position == 0, tail, head), "rng", [(0, 1), (1, 0)])
    else:
        ends = rng_count - 1
        below = lax.ppermute(tail, "rng", [(i, i + 1) for i in range(ends)])
        above = lax.ppermute(head, "rng", [(i + 1, i) for i in range(ends)])
    flags = jnp.stack([position == 0, position == rng_count - 1]).astype(jnp.int32)
    return despeckle(chunks, cells, below, above, flags)


def solution(mesh):
    in_specs = (P(None, ("sub", "rng"), None), P(), P(), P())
    out_specs = P("sub", "rng")
    return jax.shard_map(
        per_device, mesh=mesh, in_specs=in_specs, out_specs=out_specs, check_vma=False
    )
```

```python
import functools
import math
import typing

import jax
import jax.numpy as jnp
import numpy as np
from jax import lax
from jax.experimental import pallas as pl
from jax.experimental.pallas import tpu as pltpu
from jax.sharding import PartitionSpec as P

FACTOR = 64
ANG = 256
MERGES = 4
SWEEPS = 8

inv_root_two = 0.7071067811865476
phase_period = 8192

GROUP = 1 << MERGES
ROWS = 16
LANES = 128
diffusion_scale = math.sqrt(0.5)

VMEM_BYTES = 56 << 20

ANY = pl.BlockSpec(memory_space=pl.ANY)
SMEM = pl.BlockSpec(memory_space=pltpu.SMEM)
VMEM = pl.BlockSpec(memory_space=pltpu.VMEM)


def bf16(table):
    return np.asarray(table, np.float32).astype(jnp.bfloat16)


def chunked(bins):
    eighth = bins // 8
    if eighth % ROWS:
        return (((0, bins),),)
    return ((0, 3 * eighth), (6 * eighth, 2 * eighth)), ((3 * eighth, 3 * eighth),)


def length(segments):
    return sum(count for _, count in segments)


def transform_tables(segments, col_count, rng_count, norm_scale):
    index = np.arange(col_count)
    angle = 2.0 * np.pi / col_count * (np.outer(index, index) % col_count)
    cosine, sine = np.cos(angle) * norm_scale, np.sin(angle) * norm_scale
    real_rows = np.concatenate([cosine, sine], axis=1)
    imag_rows = np.concatenate([-sine, cosine], axis=1)
    swath = col_count // rng_count
    parts = [
        part[r * swath + start : r * swath + start + count]
        for r in range(rng_count)
        for part in (real_rows, imag_rows)
        for start, count in segments
    ]
    twist = 2.0 * np.pi / (GROUP * col_count) * np.outer(np.arange(GROUP), index)
    return bf16(np.concatenate(parts)), np.stack([np.cos(twist), np.sin(twist)]).astype(np.float32)


def beam_table(leaf_pulses, rng_count):
    wrapped = np.outer(np.arange(ANG) - ANG // 2, np.arange(leaf_pulses)) % leaf_pulses
    angles = 2.0 * np.pi / leaf_pulses * wrapped
    norm_scale = 1.0 / math.sqrt(leaf_pulses)
    cosine, sine = np.cos(angles).T * norm_scale, np.sin(angles).T * norm_scale
    from_real = np.concatenate([cosine, -sine], axis=1)
    from_imag = np.concatenate([sine, cosine], axis=1)
    rows = leaf_pulses // rng_count
    parts = [f[r * rows : (r + 1) * rows] for r in range(rng_count) for f in (from_real, from_imag)]
    return bf16(np.concatenate(parts))


def turned(value, numerator, denominator):
    real, imag = value
    eighth = numerator * 8 % (8 * denominator) / denominator
    if eighth == 0:
        return real, imag
    if eighth == 2:
        return imag, -real
    if eighth == 1:
        return (real + imag) * inv_root_two, (imag - real) * inv_root_two
    if eighth == 3:
        return (imag - real) * inv_root_two, -(real + imag) * inv_root_two
    angle = 2.0 * math.pi * numerator / denominator
    c, s = math.cos(angle), math.sin(angle)
    return real * c + imag * s, imag * c - real * s


def small_transform(values):
    count = len(values)
    if count == 1:
        return values
    even, odd = small_transform(values[0::2]), small_transform(values[1::2])
    low, high = [], []
    for j in range(count // 2):
        real, imag = turned(odd[j], j, count)
        low.append((even[j][0] + real, even[j][1] + imag))
        high.append((even[j][0] - real, even[j][1] - imag))
    return low + high


def transform_kernel(raw_hbm, matrix_hbm, twist_hbm, out_hbm, *refs):
    raw_ref, matrix_ref, twist_ref, stage_ref, out_ref, raw_sems, table_sems, out_sems = refs
    col_count = raw_ref.shape[2] // GROUP
    pulses = raw_ref.shape[1]
    blocks = raw_sems.shape[0]
    block = pulses // blocks
    pair = 2

    def fetch(i):
        rows = pl.ds(pl.multiple_of(i * block, block), block)
        return pltpu.make_async_copy(raw_hbm.at[:, rows], raw_ref.at[:, rows], raw_sems.at[i])

    def send(step):
        here = pl.ds(step * pair, pair)
        return pltpu.make_async_copy(out_ref.at[here], out_hbm.at[here], out_sems.at[step])

    matrix_copy = pltpu.make_async_copy(matrix_hbm, matrix_ref, table_sems.at[0])
    twist_copy = pltpu.make_async_copy(twist_hbm, twist_ref, table_sems.at[1])
    for i in range(blocks):
        fetch(i).start()
        if i == 0:
            twist_copy.start()
    matrix_copy.start()
    twist_copy.wait()

    @pl.loop(0, blocks)
    def _(i):
        fetch(i).wait()

        @pl.loop(0, block // ROWS)
        def _(step):
            rows = pl.ds(pl.multiple_of(i * block + step * ROWS, ROWS), ROWS)
            for lane in range(0, col_count, LANES):
                values = []
                for a in range(GROUP):
                    cols = pl.ds(a * col_count + lane, LANES)
                    values.append(tuple(raw_ref[part, rows, cols].astype(jnp.float32) for part in range(2)))
                for c, (real, imag) in enumerate(small_transform(values)):
                    if c:
                        cos = twist_ref[0, c : c + 1, lane : lane + LANES]
                        sin = twist_ref[1, c : c + 1, lane : lane + LANES]
                        real, imag = real * cos + imag * sin, imag * cos - real * sin
                    stage_ref[c, rows, lane : lane + LANES] = real.astype(jnp.bfloat16)
                    stage_ref[c, rows, col_count + lane : col_count + lane + LANES] = imag.astype(jnp.bfloat16)

    matrix_copy.wait()

    @pl.loop(0, GROUP // pair)
    def _(step):
        held = stage_ref[pl.ds(step * pair, pair)].reshape(pair * pulses, 2 * col_count)
        mixed = lax.dot_general(
            matrix_ref[...], held, (((1,), (1,)), ((), ())), preferred_element_type=jnp.float32
        ).astype(jnp.bfloat16)
        for j in range(pair):
            out_ref[step * pair + j] = mixed[:, j * pulses : (j + 1) * pulses]
        send(step).start()

    for step in range(GROUP // pair):
        send(step).wait()


def range_transform(segments, raw_echoes, rng_count):
    pulses, samples = raw_echoes.shape[1:]
    col_count = samples // GROUP
    matrix, twist = transform_tables(segments, col_count, rng_count, 1.0 / FACTOR)
    shape = (GROUP, rng_count * 2 * length(segments), pulses)
    return pl.pallas_call(
        transform_kernel,
        in_specs=[ANY, ANY, ANY],
        out_specs=ANY,
        out_shape=jax.ShapeDtypeStruct(shape, jnp.bfloat16),
        scratch_shapes=[
            pltpu.VMEM(raw_echoes.shape, jnp.bfloat16),
            pltpu.VMEM(matrix.shape, jnp.bfloat16),
            pltpu.VMEM(twist.shape, jnp.float32),
            pltpu.VMEM((GROUP, pulses, 2 * col_count), jnp.bfloat16),
            pltpu.VMEM(shape, jnp.bfloat16),
            pltpu.SemaphoreType.DMA((pulses // (2 * ROWS),)),
            pltpu.SemaphoreType.DMA((2,)),
            pltpu.SemaphoreType.DMA((GROUP // 2,)),
        ],
        compiler_params=pltpu.CompilerParams(vmem_limit_bytes=VMEM_BYTES),
        name="range_transform",
    )(raw_echoes, jnp.asarray(matrix), jnp.asarray(twist))


def unit_turn(steps):
    quarter = phase_period // 4
    turn = (steps + quarter // 2) // quarter
    x = (steps - turn * quarter).astype(jnp.float32) * (2.0 * math.pi / phase_period)
    x2 = x * x
    cos = 1.0 + x2 * (-1 / 2 + x2 * (1 / 24 + x2 * (-1 / 720 + x2 * (1 / 40320 + x2 * (-1 / 3628800)))))
    sin = x + x * (x2 * (-1 / 6 + x2 * (1 / 120 + x2 * (-1 / 5040 + x2 * (1 / 362880)))))
    odd = turn % 2 == 1
    cos, sin = jnp.where(odd, sin, cos), jnp.where(odd, cos, sin)
    cos = jnp.where((turn == 1) | (turn == 2), -cos, cos)
    sin = jnp.where((turn == 2) | (turn == 3), -sin, sin)
    return cos, sin


def tables_kernel(place_ref, offsets_ref, taps_ref, weights_ref, interp_ref, base_ref, step_ref):
    tap_count = taps_ref.shape[1]
    chunk = 64
    wide = taps_ref.shape[2]

    @pl.loop(0, taps_ref.shape[0])
    def _(matrix):
        for lane in range(0, wide, LANES):
            cols = slice(lane, lane + LANES)
            for a in range(0, ANG, chunk):
                index = lax.broadcasted_iota(jnp.int32, (chunk, LANES), 0) + a
                summed = jnp.zeros((chunk, LANES), jnp.float32)
                for t in range(tap_count):
                    taps = taps_ref[matrix, t : t + 1, cols]
                    summed = summed + jnp.where(taps == index, weights_ref[matrix, t : t + 1, cols], 0.0)
                interp_ref[matrix, a : a + chunk, cols] = summed.astype(jnp.bfloat16)

    first_bin = place_ref[0]
    first_leaf = place_ref[1]
    for level in range(MERGES):

        @pl.loop(0, GROUP)
        def _(leaf):
            sector = jnp.int32(0)
            for j in range(level):
                sector = sector * 2 + (leaf >> j & 1)
            offset = offsets_ref[level, first_leaf + leaf]
            where = level * GROUP + leaf
            for lane in range(0, wide, LANES):
                cols = slice(lane, lane + LANES)
                angle = sector * wide + lane + lax.broadcasted_iota(jnp.int32, (8, LANES), 1)
                per_bin = offset * angle % phase_period
                bins = first_bin + GROUP * lax.broadcasted_iota(jnp.int32, (8, LANES), 0)
                cos, sin = unit_turn(per_bin * bins % phase_period)
                base_ref[where, 0, :, cols] = cos * inv_root_two
                base_ref[where, 1, :, cols] = sin * inv_root_two
                cos, sin = unit_turn(per_bin[:1] * (GROUP * 8) % phase_period)
                step_ref[where, 0:1, cols] = cos
                step_ref[where, 1:2, cols] = sin


def merge_tables(merge_taps, merge_weights, track_offsets, place):
    level_halves = 2 * MERGES
    taps = merge_taps.reshape(level_halves, *merge_taps.shape[2:])
    weights = merge_weights.reshape(level_halves, *merge_taps.shape[2:])
    wide = 2 * ANG
    return pl.pallas_call(
        tables_kernel,
        in_specs=[SMEM, SMEM, VMEM, VMEM],
        out_shape=(
            jax.ShapeDtypeStruct((level_halves, ANG, wide), jnp.bfloat16),
            jax.ShapeDtypeStruct((MERGES * GROUP, 2, 8, wide), jnp.float32),
            jax.ShapeDtypeStruct((MERGES * GROUP, 2, wide), jnp.float32),
        ),
        compiler_params=pltpu.CompilerParams(vmem_limit_bytes=VMEM_BYTES),
        name="merge_tables",
    )(place, track_offsets, taps, weights)


def product(a, b):
    return a[0] * b[0] - a[1] * b[1], a[0] * b[1] + a[1] * b[0]


def power(a, count):
    if count == 1:
        return a
    half = power(a, count // 2)
    whole = product(half, half)
    return product(whole, a) if count % 2 else whole


def merge_kernel(segments, pulses_hbm, beam_hbm, interp_hbm, base_hbm, step_hbm, out_hbm, *refs):
    pulses_ref, beam_ref, interp_ref, base_ref, step_ref, out_ref, image_ref, mixed_ref = refs[:8]
    pulse_sems, whole_sems, level_sems, out_sems = refs[8:]
    bins = pulses_ref.shape[2]
    parts = pulses_ref.shape[1]
    batch = 4

    def copy(source, target, here, sem):
        return pltpu.make_async_copy(source.at[here], target.at[here], sem)

    def pulses_copy(i):
        return copy(pulses_hbm, pulses_ref, pl.ds(i * batch, batch), pulse_sems.at[i])

    def level_copies(level):
        return (
            copy(interp_hbm, interp_ref, pl.ds(2 * level, 2), level_sems.at[level, 0]),
            copy(base_hbm, base_ref, pl.ds(level * GROUP, GROUP), level_sems.at[level, 1]),
        )

    def out_copy(leaf):
        return copy(out_ref, out_hbm, pl.ds(leaf, 1), out_sems.at[leaf])

    beam_copy = pltpu.make_async_copy(beam_hbm, beam_ref, whole_sems.at[0])
    step_copy = pltpu.make_async_copy(step_hbm, step_ref, whole_sems.at[1])
    beam_copy.start()
    for i in range(GROUP // batch):
        pulses_copy(i).start()
    step_copy.start()
    for level in range(MERGES):
        for item in level_copies(level):
            item.start()
    beam_copy.wait()

    @pl.loop(0, GROUP // batch)
    def _(step):
        pulses_copy(step).wait()
        leaves = pl.ds(step * batch, batch)
        held = jnp.concatenate(
            [pulses_ref[leaves, j].reshape(batch * bins, pulses_ref.shape[3]) for j in range(parts)], axis=1
        )
        formed = jnp.dot(held, beam_ref[...], preferred_element_type=jnp.float32).astype(jnp.bfloat16)
        for j in range(batch):
            rows = formed[j * bins : (j + 1) * bins]
            image_ref[step * batch + j, :bins] = rows[:, :ANG]
            image_ref[step * batch + j, bins:] = rows[:, ANG:]

    step_copy.wait()
    for level in range(MERGES):
        for item in level_copies(level):
            item.wait()

        def lower(index):
            return (index >> level << (level + 1)) | (index & ((1 << level) - 1))

        @pl.loop(0, GROUP // 2 // batch)
        def _(step):
            for side in range(2):
                leaves = [lower(step * batch + j) + (side << level) for j in range(batch)]
                held = jnp.concatenate([image_ref[leaf] for leaf in leaves])
                mixed = jnp.dot(held, interp_ref[2 * level + side], preferred_element_type=jnp.float32)
                for j in range(batch):
                    mixed_ref[side, step * batch + j] = mixed[j * 2 * bins : (j + 1) * 2 * bins]

        @pl.loop(0, GROUP // 2)
        def _(index):
            low = lower(index)
            pair = (low, low + (1 << level))
            for lane in range(0, 2 * ANG, 2 * LANES):
                cols = slice(lane, lane + 2 * LANES)
                turns, steps = [], []
                for side in range(2):
                    where = level * GROUP + pair[side]
                    base = tuple(base_ref[where, part, :, cols] for part in range(2))
                    step = tuple(step_ref[where, part : part + 1, cols] for part in range(2))
                    later = product(base, step)
                    turns.append(tuple(jnp.concatenate([base[part], later[part]]) for part in range(2)))
                    steps.append(product(step, step))
                target = pair[lane // ANG]
                place = 0
                spots = [start + i for start, count in segments for i in range(0, count, ROWS)]
                for row, spot in zip(range(0, bins, ROWS), spots):
                    if spot != place:
                        jumps = [power(steps[side], (spot - place) // ROWS) for side in range(2)]
                        turns = [product(turns[side], jumps[side]) for side in range(2)]
                        place = spot
                    real, imag = 0.0, 0.0
                    for side in range(2):
                        held = tuple(
                            mixed_ref[side, index, part * bins + row : part * bins + row + ROWS, cols]
                            for part in range(2)
                        )
                        r, i = product(turns[side], held)
                        real, imag = real + r, imag + i
                    if level == MERGES - 1:
                        out_ref[target, row : row + ROWS, :] = jnp.sqrt(real * real + imag * imag).astype(
                            out_ref.dtype
                        )
                    else:
                        image_ref[target, row : row + ROWS, :] = real.astype(jnp.bfloat16)
                        image_ref[target, bins + row : bins + row + ROWS, :] = imag.astype(jnp.bfloat16)
            if level == MERGES - 1:
                for leaf in pair:
                    out_copy(leaf).start()

    for leaf in range(GROUP):
        out_copy(leaf).wait()


def merged_magnitude(segments, pulses, beam, interp, base, step):
    bins = pulses.shape[2]
    inputs = (pulses, beam, interp, base, step)
    return pl.pallas_call(
        functools.partial(merge_kernel, segments),
        in_specs=[ANY] * len(inputs),
        out_specs=ANY,
        out_shape=jax.ShapeDtypeStruct((GROUP, bins, ANG), jnp.bfloat16),
        scratch_shapes=[
            *[pltpu.VMEM(array.shape, array.dtype) for array in inputs],
            pltpu.VMEM((GROUP, bins, ANG), jnp.bfloat16),
            pltpu.VMEM((GROUP, 2 * bins, ANG), jnp.bfloat16),
            pltpu.VMEM((2, GROUP // 2, 2 * bins, 2 * ANG), jnp.float32),
            pltpu.SemaphoreType.DMA((GROUP // 4,)),
            pltpu.SemaphoreType.DMA((2,)),
            pltpu.SemaphoreType.DMA((MERGES, 2)),
            pltpu.SemaphoreType.DMA((GROUP,)),
        ],
        compiler_params=pltpu.CompilerParams(vmem_limit_bytes=VMEM_BYTES),
        name="merged_magnitude",
    )(*inputs)


class Zone(typing.NamedTuple):
    pieces: tuple
    rows: int
    begin: int
    count: int
    place: int
    below: bool
    above: bool


def zones_of(chunks, bins):
    if len(chunks) == 1:
        return (Zone(((0, 0, bins, 8),), bins, 0, bins, 0, True, True),), ()
    (_, low), (high, top) = chunks[0]
    early = (
        Zone(((0, 0, low, 8),), low, 0, low - 8, 0, True, False),
        Zone(((0, low, top, 8),), top, 8, top - 8, high + 8, False, True),
    )
    middle = bins - low - top
    pieces = ((0, low - ROWS, ROWS, 0), (1, 0, middle, ROWS), (0, low, ROWS, ROWS + middle))
    late = (Zone(pieces, middle + 16, 0, middle + 16, low - 8, False, False),)
    return early, late


def diffuse_kernel(zones, array_count, *refs):
    cells_hbms, out_hbm, scratch = refs[:array_count], refs[-1 - scratch_count(zones)], refs[-scratch_count(zones) :]
    halo_hbms = refs[array_count : array_count + 2] if any(zone.below or zone.above for zone in zones) else ()
    position = lax.axis_index("rng")
    first, last = position == 0, position == lax.axis_size("rng") - 1
    half = GROUP // 2
    blocks = [slice(h * LANES, (h + 1) * LANES) for h in range(ANG // LANES)]
    sublane = lax.broadcasted_iota(jnp.int32, (8, LANES), 0)
    held_zones = []
    if halo_hbms:
        (below_ref, above_ref, halo_sems), scratch = scratch[:3], scratch[3:]
        halo_copies = [
            pltpu.make_async_copy(halo_hbms[0], below_ref, halo_sems.at[0]),
            pltpu.make_async_copy(halo_hbms[1], above_ref, halo_sems.at[1]),
        ]
        for item in halo_copies:
            item.start()
    for zone in zones:
        pieces, scratch = scratch[: len(zone.pieces)], scratch[len(zone.pieces) :]
        out_ref, ping_ref, pong_ref, in_sems, out_sems = scratch[:5]
        scratch = scratch[5:]
        copies = [
            pltpu.make_async_copy(cells_hbms[array].at[:, pl.ds(source, rows)], pieces[k], in_sems.at[k])
            for k, (array, source, rows, _) in enumerate(zone.pieces)
        ]
        for item in copies:
            item.start()
        held_zones.append((zone, pieces, copies, out_ref, ping_ref, pong_ref, out_sems))

    def flux(upper, lower):
        difference = upper - lower
        return difference / (2.0 + difference * difference)

    sends = []
    for zone, pieces, copies, out_ref, ping_ref, pong_ref, out_sems in held_zones:
        bins = zone.rows
        pitch = bins + 16
        for (_, _, rows, start), piece, item in zip(zone.pieces, pieces, copies):
            item.wait()
            for h, cols in enumerate(blocks):
                for c in range(GROUP):
                    ping_ref[h, pl.ds(c * pitch + start, rows)] = (
                        piece[c, :, cols].astype(jnp.float32) * diffusion_scale
                    )
        if halo_hbms and zone is zones[0]:
            for item in halo_copies:
                item.wait()
        for h, cols in enumerate(blocks):
            for j in range(half):
                if zone.below:
                    down = half + j
                    own = ping_ref[h, pl.ds((GROUP - 1 - down) * pitch + 8, 1)]
                    sent = below_ref[j : j + 1, cols].astype(jnp.float32) * diffusion_scale
                    ping_ref[h, pl.ds(down * pitch + 7, 1)] = jnp.where(first, own, sent)
                if zone.above:
                    own = ping_ref[h, pl.ds((GROUP - 1 - j) * pitch + 7 + bins, 1)]
                    sent = above_ref[j : j + 1, cols].astype(jnp.float32) * diffusion_scale
                    ping_ref[h, pl.ds(j * pitch + 8 + bins, 1)] = jnp.where(last, own, sent)

        def tile(source, target, h, row, begin, end):
            def cells(c, shift=0):
                return source[h, pl.ds(c * pitch + row + shift, 8)]

            def before():
                near, far = pltpu.roll(cells(GROUP - 1), 1, 0), pltpu.roll(cells(GROUP - 1, -8), 1, 0)
                return jnp.where(sublane == 0, far, near)

            def after():
                near, far = pltpu.roll(cells(0), 7, 0), pltpu.roll(cells(0, 8), 7, 0)
                return jnp.where(sublane == 7, far, near)

            here = cells(begin)
            flow = flux(here, before()) if begin == 0 else None
            for c in range(begin, end):
                if c < end - 1:
                    there = cells(c + 1)
                elif end == GROUP:
                    there = after()
                else:
                    there = None
                ahead = flux(there, here) if there is not None else None
                value = here
                if ahead is not None:
                    value = value + ahead
                if flow is not None:
                    value = value - flow
                target[h, pl.ds(c * pitch + row, 8)] = value
                here, flow = there, ahead

        def sweep(source, target):
            for h in range(len(blocks)):
                tile(source, target, h, 0, half, GROUP)
                tile(source, target, h, 8 + bins, 0, half)

            @pl.loop(0, bins // 8)
            def _(step):
                for h in range(len(blocks)):
                    tile(source, target, h, pl.multiple_of(8 + 8 * step, 8), 0, GROUP)

        @pl.loop(0, SWEEPS // 2)
        def _(step):
            sweep(ping_ref, pong_ref)
            sweep(pong_ref, ping_ref)

        rows = LANES // GROUP

        def out_copy(step, zone=zone, out_ref=out_ref, out_sems=out_sems):
            here = pl.ds(pl.multiple_of(step * LANES, LANES), LANES)
            there = pl.ds(pl.multiple_of(zone.place * GROUP + step * LANES, LANES), LANES)
            return pltpu.make_async_copy(out_ref.at[:, here], out_hbm.at[:, there], out_sems.at[step])

        @pl.loop(0, zone.count // rows)
        def _(step):
            for h, cols in enumerate(blocks):
                held = jnp.concatenate(
                    [
                        ping_ref[h, pl.ds(8 + zone.begin + step * rows + d, GROUP, stride=pitch)]
                        for d in range(rows)
                    ]
                )
                here = pl.ds(pl.multiple_of(step * LANES, LANES), LANES)
                out_ref[cols, here] = held.T * (1.0 / diffusion_scale)
            out_copy(step).start()

        sends.append((out_copy, zone.count // rows))

    for out_copy, count in sends:
        for step in range(count):
            out_copy(step).wait()


def scratch_count(zones):
    halo = 3 * any(zone.below or zone.above for zone in zones)
    return halo + sum(len(zone.pieces) + 5 for zone in zones)


def despeckle(zones, cells, halo, bins, started=()):
    shape = (ANG, GROUP * bins)
    scratch = []
    if halo:
        scratch += [pltpu.VMEM(part.shape, part.dtype) for part in halo] + [pltpu.SemaphoreType.DMA((2,))]
    for zone in zones:
        held = pltpu.VMEM((ANG // LANES, GROUP * (zone.rows + 16), LANES), jnp.float32)
        scratch += [
            *[pltpu.VMEM((GROUP, rows, ANG), cells[array].dtype) for array, _, rows, _ in zone.pieces],
            pltpu.VMEM((ANG, GROUP * zone.count), jnp.float32),
            held,
            held,
            pltpu.SemaphoreType.DMA((len(zone.pieces),)),
            pltpu.SemaphoreType.DMA((GROUP * zone.count // LANES,)),
        ]
    return pl.pallas_call(
        functools.partial(diffuse_kernel, zones, len(cells)),
        in_specs=[ANY] * (len(cells) + len(halo) + len(started)),
        out_specs=ANY,
        out_shape=jax.ShapeDtypeStruct(shape, jnp.float32),
        scratch_shapes=scratch,
        input_output_aliases={len(cells): 0} if started else {},
        compiler_params=pltpu.CompilerParams(vmem_limit_bytes=14 << 20),
        name="despeckle",
    )(*cells, *halo, *started)


def per_device(raw_echoes, merge_taps, merge_weights, track_offsets):
    sub_count, rng_count = lax.axis_size("sub"), lax.axis_size("rng")
    leaf, position = lax.axis_index("sub"), lax.axis_index("rng")
    pulses, samples = raw_echoes.shape[1:]
    bins = samples // (GROUP * rng_count)
    groups = [[g * GROUP + i for i in range(GROUP)] for g in range(sub_count // GROUP)]
    groups = groups if len(groups) > 1 else None

    chunks = chunked(bins)

    def regroup(block, count):
        if groups is None:
            block = block.reshape(GROUP * rng_count, 2 * count, pulses)
            block = lax.all_to_all(block, ("sub", "rng"), split_axis=0, concat_axis=0, tiled=True)
        else:
            block = block.reshape(GROUP, rng_count, 2 * count, pulses)
            block = lax.all_to_all(block, "rng", split_axis=1, concat_axis=1, tiled=True)
            block = lax.all_to_all(
                block, "sub", split_axis=0, concat_axis=0, tiled=True, axis_index_groups=groups
            )
        return block.reshape(GROUP, rng_count * 2, count, pulses)

    compressed = []
    for segments in chunks:
        if compressed:
            raw_echoes, compressed[-1] = lax.optimization_barrier((raw_echoes, compressed[-1]))
        compressed.append(range_transform(segments, raw_echoes, rng_count))
    place = jnp.stack([leaf % GROUP + 1 + position * (bins * GROUP), leaf // GROUP * GROUP]).astype(jnp.int32)
    tables = merge_tables(merge_taps, merge_weights, track_offsets, place)
    regrouped = []
    for block, segments in zip(compressed, chunks):
        if regrouped:
            block, tables, regrouped[-1] = lax.optimization_barrier((block, tables, regrouped[-1]))
        regrouped.append(regroup(block, length(segments)))
    beam = jnp.asarray(beam_table(pulses * rng_count, rng_count))
    cells = []
    for segments, block in zip(chunks, regrouped):
        magnitude = merged_magnitude(segments, block, beam, *tables)
        cells.append(
            lax.all_to_all(magnitude, "sub", split_axis=0, concat_axis=0, tiled=True, axis_index_groups=groups)
        )
    half = GROUP // 2
    head, tail = cells[0][:half, 0], cells[0][half:, -1]
    if rng_count == 2:
        below = above = lax.ppermute(jnp.where(position == 0, tail, head), "rng", [(0, 1), (1, 0)])
    else:
        ends = rng_count - 1
        below = lax.ppermute(tail, "rng", [(i, i + 1) for i in range(ends)])
        above = lax.ppermute(head, "rng", [(i + 1, i) for i in range(ends)])
    early, late = zones_of(chunks, bins)
    result = despeckle(early, cells[:1], (below, above), bins)
    if late:
        result = despeckle(late, cells, (), bins, (result,))
    return result


def solution(mesh):
    in_specs = (P(None, ("sub", "rng"), None), P(), P(), P())
    out_specs = P("sub", "rng")
    return jax.shard_map(
        per_device, mesh=mesh, in_specs=in_specs, out_specs=out_specs, check_vma=False
    )
```

```python
import functools
import math
import typing

import jax
import jax.numpy as jnp
import numpy as np
from jax import lax
from jax.experimental import pallas as pl
from jax.experimental.pallas import tpu as pltpu
from jax.sharding import PartitionSpec as P

FACTOR = 64
ANG = 256
MERGES = 4
SWEEPS = 8

inv_root_two = 0.7071067811865476
phase_period = 8192

GROUP = 1 << MERGES
ROWS = 16
LANES = 128
diffusion_scale = math.sqrt(0.5)

VMEM_BYTES = 56 << 20

ANY = pl.BlockSpec(memory_space=pl.ANY)
SMEM = pl.BlockSpec(memory_space=pltpu.SMEM)
VMEM = pl.BlockSpec(memory_space=pltpu.VMEM)


def bf16(table):
    return np.asarray(table, np.float32).astype(jnp.bfloat16)


def chunked(bins):
    eighth = bins // 8
    if eighth % ROWS:
        return (((0, bins),),)
    return ((0, 3 * eighth), (6 * eighth, 2 * eighth)), ((3 * eighth, 3 * eighth),)


def length(segments):
    return sum(count for _, count in segments)


def transform_tables(segments, col_count, rng_count, norm_scale):
    index = np.arange(col_count)
    angle = 2.0 * np.pi / col_count * (np.outer(index, index) % col_count)
    cosine, sine = np.cos(angle) * norm_scale, np.sin(angle) * norm_scale
    real_rows = np.concatenate([cosine, sine], axis=1)
    imag_rows = np.concatenate([-sine, cosine], axis=1)
    swath = col_count // rng_count
    parts = [
        part[r * swath + start : r * swath + start + count]
        for r in range(rng_count)
        for part in (real_rows, imag_rows)
        for start, count in segments
    ]
    twist = 2.0 * np.pi / (GROUP * col_count) * np.outer(np.arange(GROUP), index)
    return bf16(np.concatenate(parts)), np.stack([np.cos(twist), np.sin(twist)]).astype(np.float32)


def beam_table(leaf_pulses, rng_count):
    wrapped = np.outer(np.arange(ANG) - ANG // 2, np.arange(leaf_pulses)) % leaf_pulses
    angles = 2.0 * np.pi / leaf_pulses * wrapped
    norm_scale = 1.0 / math.sqrt(leaf_pulses)
    cosine, sine = np.cos(angles).T * norm_scale, np.sin(angles).T * norm_scale
    from_real = np.concatenate([cosine, -sine], axis=1)
    from_imag = np.concatenate([sine, cosine], axis=1)
    rows = leaf_pulses // rng_count
    parts = [f[r * rows : (r + 1) * rows] for r in range(rng_count) for f in (from_real, from_imag)]
    return bf16(np.concatenate(parts))


def turned(value, numerator, denominator):
    real, imag = value
    eighth = numerator * 8 % (8 * denominator) / denominator
    if eighth == 0:
        return real, imag
    if eighth == 2:
        return imag, -real
    if eighth == 1:
        return (real + imag) * inv_root_two, (imag - real) * inv_root_two
    if eighth == 3:
        return (imag - real) * inv_root_two, -(real + imag) * inv_root_two
    angle = 2.0 * math.pi * numerator / denominator
    c, s = math.cos(angle), math.sin(angle)
    return real * c + imag * s, imag * c - real * s


def small_transform(values):
    count = len(values)
    if count == 1:
        return values
    even, odd = small_transform(values[0::2]), small_transform(values[1::2])
    low, high = [], []
    for j in range(count // 2):
        real, imag = turned(odd[j], j, count)
        low.append((even[j][0] + real, even[j][1] + imag))
        high.append((even[j][0] - real, even[j][1] - imag))
    return low + high


def transform_kernel(raw_hbm, matrix_hbm, twist_hbm, out_hbm, *refs):
    raw_ref, matrix_ref, twist_ref, stage_ref, out_ref, raw_sems, table_sems, out_sems = refs
    col_count = raw_ref.shape[2] // GROUP
    pulses = raw_ref.shape[1]
    blocks = raw_sems.shape[0]
    block = pulses // blocks
    pair = 2

    def fetch(i):
        rows = pl.ds(pl.multiple_of(i * block, block), block)
        return pltpu.make_async_copy(raw_hbm.at[:, rows], raw_ref.at[:, rows], raw_sems.at[i])

    def send(step):
        here = pl.ds(step * pair, pair)
        return pltpu.make_async_copy(out_ref.at[here], out_hbm.at[here], out_sems.at[step])

    matrix_copy = pltpu.make_async_copy(matrix_hbm, matrix_ref, table_sems.at[0])
    twist_copy = pltpu.make_async_copy(twist_hbm, twist_ref, table_sems.at[1])
    for i in range(blocks):
        fetch(i).start()
        if i == 0:
            twist_copy.start()
    matrix_copy.start()
    twist_copy.wait()

    @pl.loop(0, blocks)
    def _(i):
        fetch(i).wait()

        @pl.loop(0, block // ROWS)
        def _(step):
            rows = pl.ds(pl.multiple_of(i * block + step * ROWS, ROWS), ROWS)
            for lane in range(0, col_count, LANES):
                values = []
                for a in range(GROUP):
                    cols = pl.ds(a * col_count + lane, LANES)
                    values.append(tuple(raw_ref[part, rows, cols].astype(jnp.float32) for part in range(2)))
                for c, (real, imag) in enumerate(small_transform(values)):
                    if c:
                        cos = twist_ref[0, c : c + 1, lane : lane + LANES]
                        sin = twist_ref[1, c : c + 1, lane : lane + LANES]
                        real, imag = real * cos + imag * sin, imag * cos - real * sin
                    stage_ref[c, rows, lane : lane + LANES] = real.astype(jnp.bfloat16)
                    stage_ref[c, rows, col_count + lane : col_count + lane + LANES] = imag.astype(jnp.bfloat16)

    matrix_copy.wait()

    @pl.loop(0, GROUP // pair)
    def _(step):
        held = stage_ref[pl.ds(step * pair, pair)].reshape(pair * pulses, 2 * col_count)
        mixed = lax.dot_general(
            matrix_ref[...], held, (((1,), (1,)), ((), ())), preferred_element_type=jnp.float32
        ).astype(jnp.bfloat16)
        for j in range(pair):
            out_ref[step * pair + j] = mixed[:, j * pulses : (j + 1) * pulses]
        send(step).start()

    for step in range(GROUP // pair):
        send(step).wait()


def range_transform(segments, raw_echoes, rng_count):
    pulses, samples = raw_echoes.shape[1:]
    col_count = samples // GROUP
    matrix, twist = transform_tables(segments, col_count, rng_count, 1.0 / FACTOR)
    shape = (GROUP, rng_count * 2 * length(segments), pulses)
    return pl.pallas_call(
        transform_kernel,
        in_specs=[ANY, ANY, ANY],
        out_specs=ANY,
        out_shape=jax.ShapeDtypeStruct(shape, jnp.bfloat16),
        scratch_shapes=[
            pltpu.VMEM(raw_echoes.shape, jnp.bfloat16),
            pltpu.VMEM(matrix.shape, jnp.bfloat16),
            pltpu.VMEM(twist.shape, jnp.float32),
            pltpu.VMEM((GROUP, pulses, 2 * col_count), jnp.bfloat16),
            pltpu.VMEM(shape, jnp.bfloat16),
            pltpu.SemaphoreType.DMA((pulses // (2 * ROWS),)),
            pltpu.SemaphoreType.DMA((2,)),
            pltpu.SemaphoreType.DMA((GROUP // 2,)),
        ],
        compiler_params=pltpu.CompilerParams(vmem_limit_bytes=VMEM_BYTES),
        name="range_transform",
    )(raw_echoes, jnp.asarray(matrix), jnp.asarray(twist))


def unit_turn(steps):
    quarter = phase_period // 4
    turn = (steps + quarter // 2) // quarter
    x = (steps - turn * quarter).astype(jnp.float32) * (2.0 * math.pi / phase_period)
    x2 = x * x
    cos = 1.0 + x2 * (-1 / 2 + x2 * (1 / 24 + x2 * (-1 / 720 + x2 * (1 / 40320 + x2 * (-1 / 3628800)))))
    sin = x + x * (x2 * (-1 / 6 + x2 * (1 / 120 + x2 * (-1 / 5040 + x2 * (1 / 362880)))))
    odd = turn % 2 == 1
    cos, sin = jnp.where(odd, sin, cos), jnp.where(odd, cos, sin)
    cos = jnp.where((turn == 1) | (turn == 2), -cos, cos)
    sin = jnp.where((turn == 2) | (turn == 3), -sin, sin)
    return cos, sin


def tables_kernel(place_ref, offsets_ref, taps_ref, weights_ref, interp_ref, base_ref, step_ref):
    tap_count = taps_ref.shape[1]
    chunk = 64
    wide = taps_ref.shape[2]

    @pl.loop(0, taps_ref.shape[0])
    def _(matrix):
        for lane in range(0, wide, LANES):
            cols = slice(lane, lane + LANES)
            for a in range(0, ANG, chunk):
                index = lax.broadcasted_iota(jnp.int32, (chunk, LANES), 0) + a
                summed = jnp.zeros((chunk, LANES), jnp.float32)
                for t in range(tap_count):
                    taps = taps_ref[matrix, t : t + 1, cols]
                    summed = summed + jnp.where(taps == index, weights_ref[matrix, t : t + 1, cols], 0.0)
                interp_ref[matrix, a : a + chunk, cols] = summed.astype(jnp.bfloat16)

    first_bin = place_ref[0]
    first_leaf = place_ref[1]
    for level in range(MERGES):

        @pl.loop(0, GROUP)
        def _(leaf):
            sector = jnp.int32(0)
            for j in range(level):
                sector = sector * 2 + (leaf >> j & 1)
            offset = offsets_ref[level, first_leaf + leaf]
            where = level * GROUP + leaf
            for lane in range(0, wide, LANES):
                cols = slice(lane, lane + LANES)
                angle = sector * wide + lane + lax.broadcasted_iota(jnp.int32, (8, LANES), 1)
                per_bin = offset * angle % phase_period
                bins = first_bin + GROUP * lax.broadcasted_iota(jnp.int32, (8, LANES), 0)
                cos, sin = unit_turn(per_bin * bins % phase_period)
                base_ref[where, 0, :, cols] = cos * inv_root_two
                base_ref[where, 1, :, cols] = sin * inv_root_two
                cos, sin = unit_turn(per_bin[:1] * (GROUP * 8) % phase_period)
                step_ref[where, 0:1, cols] = cos
                step_ref[where, 1:2, cols] = sin


def merge_tables(merge_taps, merge_weights, track_offsets, place):
    level_halves = 2 * MERGES
    taps = merge_taps.reshape(level_halves, *merge_taps.shape[2:])
    weights = merge_weights.reshape(level_halves, *merge_taps.shape[2:])
    wide = 2 * ANG
    return pl.pallas_call(
        tables_kernel,
        in_specs=[SMEM, SMEM, VMEM, VMEM],
        out_shape=(
            jax.ShapeDtypeStruct((level_halves, ANG, wide), jnp.bfloat16),
            jax.ShapeDtypeStruct((MERGES * GROUP, 2, 8, wide), jnp.float32),
            jax.ShapeDtypeStruct((MERGES * GROUP, 2, wide), jnp.float32),
        ),
        compiler_params=pltpu.CompilerParams(vmem_limit_bytes=VMEM_BYTES),
        name="merge_tables",
    )(place, track_offsets, taps, weights)


def product(a, b):
    return a[0] * b[0] - a[1] * b[1], a[0] * b[1] + a[1] * b[0]


def power(a, count):
    if count == 1:
        return a
    half = power(a, count // 2)
    whole = product(half, half)
    return product(whole, a) if count % 2 else whole


def merge_kernel(segments, pulses_hbm, beam_hbm, interp_hbm, base_hbm, step_hbm, out_hbm, *refs):
    pulses_ref, beam_ref, interp_ref, base_ref, step_ref, out_ref, image_ref, mixed_ref = refs[:8]
    pulse_sems, whole_sems, level_sems, out_sems = refs[8:]
    bins = pulses_ref.shape[2]
    parts = pulses_ref.shape[1]
    batch = 4

    def copy(source, target, here, sem):
        return pltpu.make_async_copy(source.at[here], target.at[here], sem)

    def pulses_copy(i):
        return copy(pulses_hbm, pulses_ref, pl.ds(i * batch, batch), pulse_sems.at[i])

    def level_copies(level):
        return (
            copy(interp_hbm, interp_ref, pl.ds(2 * level, 2), level_sems.at[level, 0]),
            copy(base_hbm, base_ref, pl.ds(level * GROUP, GROUP), level_sems.at[level, 1]),
        )

    def out_copy(leaf):
        return copy(out_ref, out_hbm, pl.ds(leaf, 1), out_sems.at[leaf])

    beam_copy = pltpu.make_async_copy(beam_hbm, beam_ref, whole_sems.at[0])
    step_copy = pltpu.make_async_copy(step_hbm, step_ref, whole_sems.at[1])
    beam_copy.start()
    for i in range(GROUP // batch):
        pulses_copy(i).start()
    step_copy.start()
    for level in range(MERGES):
        for item in level_copies(level):
            item.start()
    beam_copy.wait()

    @pl.loop(0, GROUP // batch)
    def _(step):
        pulses_copy(step).wait()
        leaves = pl.ds(step * batch, batch)
        held = jnp.concatenate(
            [pulses_ref[leaves, j].reshape(batch * bins, pulses_ref.shape[3]) for j in range(parts)], axis=1
        )
        formed = jnp.dot(held, beam_ref[...], preferred_element_type=jnp.float32).astype(jnp.bfloat16)
        for j in range(batch):
            rows = formed[j * bins : (j + 1) * bins]
            image_ref[step * batch + j, :bins] = rows[:, :ANG]
            image_ref[step * batch + j, bins:] = rows[:, ANG:]

    step_copy.wait()
    for level in range(MERGES):
        for item in level_copies(level):
            item.wait()

        def lower(index):
            return (index >> level << (level + 1)) | (index & ((1 << level) - 1))

        @pl.loop(0, GROUP // 2 // batch)
        def _(step):
            for side in range(2):
                leaves = [lower(step * batch + j) + (side << level) for j in range(batch)]
                held = jnp.concatenate([image_ref[leaf] for leaf in leaves])
                mixed = jnp.dot(held, interp_ref[2 * level + side], preferred_element_type=jnp.float32)
                for j in range(batch):
                    mixed_ref[side, step * batch + j] = mixed[j * 2 * bins : (j + 1) * 2 * bins]

        @pl.loop(0, GROUP // 2)
        def _(index):
            low = lower(index)
            pair = (low, low + (1 << level))
            for lane in range(0, 2 * ANG, 2 * LANES):
                cols = slice(lane, lane + 2 * LANES)
                turns, steps = [], []
                for side in range(2):
                    where = level * GROUP + pair[side]
                    base = tuple(base_ref[where, part, :, cols] for part in range(2))
                    step = tuple(step_ref[where, part : part + 1, cols] for part in range(2))
                    later = product(base, step)
                    turns.append(tuple(jnp.concatenate([base[part], later[part]]) for part in range(2)))
                    steps.append(product(step, step))
                target = pair[lane // ANG]
                place = 0
                spots = [start + i for start, count in segments for i in range(0, count, ROWS)]
                for row, spot in zip(range(0, bins, ROWS), spots):
                    if spot != place:
                        jumps = [power(steps[side], (spot - place) // ROWS) for side in range(2)]
                        turns = [product(turns[side], jumps[side]) for side in range(2)]
                        place = spot
                    real, imag = 0.0, 0.0
                    for side in range(2):
                        held = tuple(
                            mixed_ref[side, index, part * bins + row : part * bins + row + ROWS, cols]
                            for part in range(2)
                        )
                        r, i = product(turns[side], held)
                        real, imag = real + r, imag + i
                    if level == MERGES - 1:
                        out_ref[target, row : row + ROWS, :] = jnp.sqrt(real * real + imag * imag).astype(
                            out_ref.dtype
                        )
                    else:
                        image_ref[target, row : row + ROWS, :] = real.astype(jnp.bfloat16)
                        image_ref[target, bins + row : bins + row + ROWS, :] = imag.astype(jnp.bfloat16)
            if level == MERGES - 1:
                for leaf in pair:
                    out_copy(leaf).start()

    for leaf in range(GROUP):
        out_copy(leaf).wait()


def merged_magnitude(segments, pulses, beam, interp, base, step):
    bins = pulses.shape[2]
    inputs = (pulses, beam, interp, base, step)
    return pl.pallas_call(
        functools.partial(merge_kernel, segments),
        in_specs=[ANY] * len(inputs),
        out_specs=ANY,
        out_shape=jax.ShapeDtypeStruct((GROUP, bins, ANG), jnp.bfloat16),
        scratch_shapes=[
            *[pltpu.VMEM(array.shape, array.dtype) for array in inputs],
            pltpu.VMEM((GROUP, bins, ANG), jnp.bfloat16),
            pltpu.VMEM((GROUP, 2 * bins, ANG), jnp.bfloat16),
            pltpu.VMEM((2, GROUP // 2, 2 * bins, 2 * ANG), jnp.float32),
            pltpu.SemaphoreType.DMA((GROUP // 4,)),
            pltpu.SemaphoreType.DMA((2,)),
            pltpu.SemaphoreType.DMA((MERGES, 2)),
            pltpu.SemaphoreType.DMA((GROUP,)),
        ],
        compiler_params=pltpu.CompilerParams(vmem_limit_bytes=VMEM_BYTES),
        name="merged_magnitude",
    )(*inputs)


class Zone(typing.NamedTuple):
    pieces: tuple
    rows: int
    begin: int
    count: int
    place: int
    below: bool
    above: bool


def zones_of(chunks, bins):
    if len(chunks) == 1:
        return (Zone(((0, 0, bins, 8),), bins, 0, bins, 0, True, True),), ()
    (_, low), (high, top) = chunks[0]
    early = (
        Zone(((0, 0, low, 8),), low, 0, low - 8, 0, True, False),
        Zone(((0, low, top, 8),), top, 8, top - 8, high + 8, False, True),
    )
    middle = bins - low - top
    pieces = ((0, low - ROWS, ROWS, 0), (1, 0, middle, ROWS), (0, low, ROWS, ROWS + middle))
    late = (Zone(pieces, middle + 16, 0, middle + 16, low - 8, False, False),)
    return early, late


def diffuse_kernel(zones, array_count, *refs):
    cells_refs, out_hbm, scratch = refs[:array_count], refs[-1 - 4 * len(zones)], refs[-4 * len(zones) :]
    halo_refs = refs[array_count : array_count + 2] if any(zone.below or zone.above for zone in zones) else ()
    position = lax.axis_index("rng")
    first, last = position == 0, position == lax.axis_size("rng") - 1
    half = GROUP // 2
    blocks = [slice(h * LANES, (h + 1) * LANES) for h in range(ANG // LANES)]
    sublane = lax.broadcasted_iota(jnp.int32, (8, LANES), 0)
    if halo_refs:
        below_ref, above_ref = halo_refs
    held_zones = []
    for k, zone in enumerate(zones):
        held_zones.append((zone, *scratch[4 * k : 4 * k + 4]))

    def flux(upper, lower):
        difference = upper - lower
        return difference / (2.0 + difference * difference)

    sends = []
    for zone, out_ref, ping_ref, pong_ref, out_sems in held_zones:
        bins = zone.rows
        pitch = bins + 16
        for array, source, rows, start in zone.pieces:
            for h, cols in enumerate(blocks):
                for c in range(GROUP):
                    ping_ref[h, pl.ds(c * pitch + start, rows)] = (
                        cells_refs[array][c, source : source + rows, cols].astype(jnp.float32) * diffusion_scale
                    )
        for h, cols in enumerate(blocks):
            for j in range(half):
                if zone.below:
                    down = half + j
                    own = ping_ref[h, pl.ds((GROUP - 1 - down) * pitch + 8, 1)]
                    sent = below_ref[j : j + 1, cols].astype(jnp.float32) * diffusion_scale
                    ping_ref[h, pl.ds(down * pitch + 7, 1)] = jnp.where(first, own, sent)
                if zone.above:
                    own = ping_ref[h, pl.ds((GROUP - 1 - j) * pitch + 7 + bins, 1)]
                    sent = above_ref[j : j + 1, cols].astype(jnp.float32) * diffusion_scale
                    ping_ref[h, pl.ds(j * pitch + 8 + bins, 1)] = jnp.where(last, own, sent)

        def tile(source, target, h, row, begin, end):
            def cells(c, shift=0):
                return source[h, pl.ds(c * pitch + row + shift, 8)]

            def before():
                near, far = pltpu.roll(cells(GROUP - 1), 1, 0), pltpu.roll(cells(GROUP - 1, -8), 1, 0)
                return jnp.where(sublane == 0, far, near)

            def after():
                near, far = pltpu.roll(cells(0), 7, 0), pltpu.roll(cells(0, 8), 7, 0)
                return jnp.where(sublane == 7, far, near)

            here = cells(begin)
            flow = flux(here, before()) if begin == 0 else None
            for c in range(begin, end):
                if c < end - 1:
                    there = cells(c + 1)
                elif end == GROUP:
                    there = after()
                else:
                    there = None
                ahead = flux(there, here) if there is not None else None
                value = here
                if ahead is not None:
                    value = value + ahead
                if flow is not None:
                    value = value - flow
                target[h, pl.ds(c * pitch + row, 8)] = value
                here, flow = there, ahead

        def sweep(source, target):
            for h in range(len(blocks)):
                if zone.below or zone.begin == 0:
                    tile(source, target, h, 0, half, GROUP)
                if zone.above or zone.begin + zone.count == bins:
                    tile(source, target, h, 8 + bins, 0, half)

            @pl.loop(0, bins // 8)
            def _(step):
                for h in range(len(blocks)):
                    tile(source, target, h, pl.multiple_of(8 + 8 * step, 8), 0, GROUP)

        @pl.loop(0, SWEEPS // 2)
        def _(step):
            sweep(ping_ref, pong_ref)
            sweep(pong_ref, ping_ref)

        rows = LANES // GROUP

        def out_copy(step, zone=zone, out_ref=out_ref, out_sems=out_sems):
            here = pl.ds(pl.multiple_of(step * LANES, LANES), LANES)
            there = pl.ds(pl.multiple_of(zone.place * GROUP + step * LANES, LANES), LANES)
            return pltpu.make_async_copy(out_ref.at[:, here], out_hbm.at[:, there], out_sems.at[step])

        @pl.loop(0, zone.count // rows)
        def _(step):
            for h, cols in enumerate(blocks):
                held = jnp.concatenate(
                    [
                        ping_ref[h, pl.ds(8 + zone.begin + step * rows + d, GROUP, stride=pitch)]
                        for d in range(rows)
                    ]
                )
                here = pl.ds(pl.multiple_of(step * LANES, LANES), LANES)
                out_ref[cols, here] = held.T * (1.0 / diffusion_scale)
            out_copy(step).start()

        sends.append((out_copy, zone.count // rows))

    for out_copy, count in sends:
        for step in range(count):
            out_copy(step).wait()


def despeckle(zones, cells, halo, bins, started=()):
    shape = (ANG, GROUP * bins)
    scratch = []
    for zone in zones:
        held = pltpu.VMEM((ANG // LANES, GROUP * (zone.rows + 16), LANES), jnp.float32)
        scratch += [
            pltpu.VMEM((ANG, GROUP * zone.count), jnp.float32),
            held,
            held,
            pltpu.SemaphoreType.DMA((GROUP * zone.count // LANES,)),
        ]
    return pl.pallas_call(
        functools.partial(diffuse_kernel, zones, len(cells)),
        in_specs=[VMEM] * (len(cells) + len(halo)) + [ANY] * len(started),
        out_specs=ANY,
        out_shape=jax.ShapeDtypeStruct(shape, jnp.float32),
        scratch_shapes=scratch,
        input_output_aliases={len(cells): 0} if started else {},
        compiler_params=pltpu.CompilerParams(vmem_limit_bytes=14 << 20),
        name="despeckle",
    )(*cells, *halo, *started)


def per_device(raw_echoes, merge_taps, merge_weights, track_offsets):
    sub_count, rng_count = lax.axis_size("sub"), lax.axis_size("rng")
    leaf, position = lax.axis_index("sub"), lax.axis_index("rng")
    pulses, samples = raw_echoes.shape[1:]
    bins = samples // (GROUP * rng_count)
    groups = [[g * GROUP + i for i in range(GROUP)] for g in range(sub_count // GROUP)]
    groups = groups if len(groups) > 1 else None

    chunks = chunked(bins)

    def regroup(block, count):
        if groups is None:
            block = block.reshape(GROUP * rng_count, 2 * count, pulses)
            block = lax.all_to_all(block, ("sub", "rng"), split_axis=0, concat_axis=0, tiled=True)
        else:
            block = block.reshape(GROUP, rng_count, 2 * count, pulses)
            block = lax.all_to_all(block, "rng", split_axis=1, concat_axis=1, tiled=True)
            block = lax.all_to_all(
                block, "sub", split_axis=0, concat_axis=0, tiled=True, axis_index_groups=groups
            )
        return block.reshape(GROUP, rng_count * 2, count, pulses)

    compressed = []
    for segments in chunks:
        if compressed:
            raw_echoes, compressed[-1] = lax.optimization_barrier((raw_echoes, compressed[-1]))
        compressed.append(range_transform(segments, raw_echoes, rng_count))
    place = jnp.stack([leaf % GROUP + 1 + position * (bins * GROUP), leaf // GROUP * GROUP]).astype(jnp.int32)
    tables = merge_tables(merge_taps, merge_weights, track_offsets, place)
    regrouped = []
    for block, segments in zip(compressed, chunks):
        if regrouped:
            block, tables, regrouped[-1] = lax.optimization_barrier((block, tables, regrouped[-1]))
        regrouped.append(regroup(block, length(segments)))
    beam = jnp.asarray(beam_table(pulses * rng_count, rng_count))
    cells = []
    for segments, block in zip(chunks, regrouped):
        magnitude = merged_magnitude(segments, block, beam, *tables)
        cells.append(
            lax.all_to_all(magnitude, "sub", split_axis=0, concat_axis=0, tiled=True, axis_index_groups=groups)
        )
    half = GROUP // 2
    head, tail = cells[0][:half, 0], cells[0][half:, -1]
    if rng_count == 2:
        below = above = lax.ppermute(jnp.where(position == 0, tail, head), "rng", [(0, 1), (1, 0)])
    else:
        ends = rng_count - 1
        below = lax.ppermute(tail, "rng", [(i, i + 1) for i in range(ends)])
        above = lax.ppermute(head, "rng", [(i + 1, i) for i in range(ends)])
    early, late = zones_of(chunks, bins)
    result = despeckle(early, cells[:1], (below, above), bins)
    if late:
        result = despeckle(late, cells, (), bins, (result,))
    return result


def solution(mesh):
    in_specs = (P(None, ("sub", "rng"), None), P(), P(), P())
    out_specs = P("sub", "rng")
    return jax.shard_map(
        per_device, mesh=mesh, in_specs=in_specs, out_specs=out_specs, check_vma=False
    )
```

```python
import functools
import math
import typing

import jax
import jax.numpy as jnp
import numpy as np
from jax import lax
from jax.experimental import pallas as pl
from jax.experimental.pallas import tpu as pltpu
from jax.sharding import PartitionSpec as P

FACTOR = 64
ANG = 256
MERGES = 4
SWEEPS = 8

inv_root_two = 0.7071067811865476
phase_period = 8192

GROUP = 1 << MERGES
ROWS = 16
LANES = 128
diffusion_scale = math.sqrt(0.5)

VMEM_BYTES = 56 << 20

ANY = pl.BlockSpec(memory_space=pl.ANY)
SMEM = pl.BlockSpec(memory_space=pltpu.SMEM)
VMEM = pl.BlockSpec(memory_space=pltpu.VMEM)


def bf16(table):
    return np.asarray(table, np.float32).astype(jnp.bfloat16)


def chunked(bins):
    eighth = bins // 8
    if eighth % ROWS:
        return (((0, bins),),)
    return ((0, 3 * eighth), (6 * eighth, 2 * eighth)), ((3 * eighth, 3 * eighth),)


def length(segments):
    return sum(count for _, count in segments)


def transform_tables(segments, col_count, rng_count, norm_scale):
    index = np.arange(col_count)
    angle = 2.0 * np.pi / col_count * (np.outer(index, index) % col_count)
    cosine, sine = np.cos(angle) * norm_scale, np.sin(angle) * norm_scale
    real_rows = np.concatenate([cosine, sine], axis=1)
    imag_rows = np.concatenate([-sine, cosine], axis=1)
    swath = col_count // rng_count
    parts = [
        part[r * swath + start : r * swath + start + count]
        for r in range(rng_count)
        for part in (real_rows, imag_rows)
        for start, count in segments
    ]
    twist = 2.0 * np.pi / (GROUP * col_count) * np.outer(np.arange(GROUP), index)
    return bf16(np.concatenate(parts)), np.stack([np.cos(twist), np.sin(twist)]).astype(np.float32)


def beam_table(leaf_pulses, rng_count):
    wrapped = np.outer(np.arange(ANG) - ANG // 2, np.arange(leaf_pulses)) % leaf_pulses
    angles = 2.0 * np.pi / leaf_pulses * wrapped
    norm_scale = 1.0 / math.sqrt(leaf_pulses)
    cosine, sine = np.cos(angles).T * norm_scale, np.sin(angles).T * norm_scale
    from_real = np.concatenate([cosine, -sine], axis=1)
    from_imag = np.concatenate([sine, cosine], axis=1)
    rows = leaf_pulses // rng_count
    parts = [f[r * rows : (r + 1) * rows] for r in range(rng_count) for f in (from_real, from_imag)]
    return bf16(np.concatenate(parts))


def turned(value, numerator, denominator):
    real, imag = value
    eighth = numerator * 8 % (8 * denominator) / denominator
    if eighth == 0:
        return real, imag
    if eighth == 2:
        return imag, -real
    if eighth == 1:
        return (real + imag) * inv_root_two, (imag - real) * inv_root_two
    if eighth == 3:
        return (imag - real) * inv_root_two, -(real + imag) * inv_root_two
    angle = 2.0 * math.pi * numerator / denominator
    c, s = math.cos(angle), math.sin(angle)
    return real * c + imag * s, imag * c - real * s


def small_transform(values):
    count = len(values)
    if count == 1:
        return values
    even, odd = small_transform(values[0::2]), small_transform(values[1::2])
    low, high = [], []
    for j in range(count // 2):
        real, imag = turned(odd[j], j, count)
        low.append((even[j][0] + real, even[j][1] + imag))
        high.append((even[j][0] - real, even[j][1] - imag))
    return low + high


def transform_kernel(raw_hbm, matrix_hbm, twist_hbm, out_hbm, *refs):
    raw_ref, matrix_ref, twist_ref, stage_ref, out_ref, raw_sems, table_sems, out_sems = refs
    col_count = raw_ref.shape[2] // GROUP
    pulses = raw_ref.shape[1]
    blocks = raw_sems.shape[0]
    block = pulses // blocks
    pair = 4

    def fetch(i):
        rows = pl.ds(pl.multiple_of(i * block, block), block)
        return pltpu.make_async_copy(raw_hbm.at[:, rows], raw_ref.at[:, rows], raw_sems.at[i])

    def send(step):
        here = pl.ds(step * pair, pair)
        return pltpu.make_async_copy(out_ref.at[here], out_hbm.at[here], out_sems.at[step])

    matrix_copy = pltpu.make_async_copy(matrix_hbm, matrix_ref, table_sems.at[0])
    twist_copy = pltpu.make_async_copy(twist_hbm, twist_ref, table_sems.at[1])
    for i in range(blocks):
        fetch(i).start()
        if i == 0:
            twist_copy.start()
    matrix_copy.start()
    twist_copy.wait()

    @pl.loop(0, blocks)
    def _(i):
        fetch(i).wait()

        @pl.loop(0, block // ROWS)
        def _(step):
            rows = pl.ds(pl.multiple_of(i * block + step * ROWS, ROWS), ROWS)
            for lane in range(0, col_count, LANES):
                values = []
                for a in range(GROUP):
                    cols = pl.ds(a * col_count + lane, LANES)
                    values.append(tuple(raw_ref[part, rows, cols].astype(jnp.float32) for part in range(2)))
                for c, (real, imag) in enumerate(small_transform(values)):
                    if c:
                        cos = twist_ref[0, c : c + 1, lane : lane + LANES]
                        sin = twist_ref[1, c : c + 1, lane : lane + LANES]
                        real, imag = real * cos + imag * sin, imag * cos - real * sin
                    stage_ref[c, rows, lane : lane + LANES] = real.astype(jnp.bfloat16)
                    stage_ref[c, rows, col_count + lane : col_count + lane + LANES] = imag.astype(jnp.bfloat16)

    matrix_copy.wait()

    @pl.loop(0, GROUP // pair)
    def _(step):
        held = stage_ref[pl.ds(step * pair, pair)].reshape(pair * pulses, 2 * col_count)
        mixed = lax.dot_general(
            matrix_ref[...], held, (((1,), (1,)), ((), ())), preferred_element_type=jnp.float32
        ).astype(jnp.bfloat16)
        for j in range(pair):
            out_ref[step * pair + j] = mixed[:, j * pulses : (j + 1) * pulses]
        send(step).start()

    for step in range(GROUP // pair):
        send(step).wait()


def range_transform(segments, raw_echoes, rng_count):
    pulses, samples = raw_echoes.shape[1:]
    col_count = samples // GROUP
    matrix, twist = transform_tables(segments, col_count, rng_count, 1.0 / FACTOR)
    shape = (GROUP, rng_count * 2 * length(segments), pulses)
    return pl.pallas_call(
        transform_kernel,
        in_specs=[ANY, ANY, ANY],
        out_specs=ANY,
        out_shape=jax.ShapeDtypeStruct(shape, jnp.bfloat16),
        scratch_shapes=[
            pltpu.VMEM(raw_echoes.shape, jnp.bfloat16),
            pltpu.VMEM(matrix.shape, jnp.bfloat16),
            pltpu.VMEM(twist.shape, jnp.float32),
            pltpu.VMEM((GROUP, pulses, 2 * col_count), jnp.bfloat16),
            pltpu.VMEM(shape, jnp.bfloat16),
            pltpu.SemaphoreType.DMA((pulses // (2 * ROWS),)),
            pltpu.SemaphoreType.DMA((2,)),
            pltpu.SemaphoreType.DMA((GROUP // 4,)),
        ],
        compiler_params=pltpu.CompilerParams(vmem_limit_bytes=VMEM_BYTES),
        name="range_transform",
    )(raw_echoes, jnp.asarray(matrix), jnp.asarray(twist))


def unit_turn(steps):
    quarter = phase_period // 4
    turn = (steps + quarter // 2) // quarter
    x = (steps - turn * quarter).astype(jnp.float32) * (2.0 * math.pi / phase_period)
    x2 = x * x
    cos = 1.0 + x2 * (-1 / 2 + x2 * (1 / 24 + x2 * (-1 / 720 + x2 * (1 / 40320 + x2 * (-1 / 3628800)))))
    sin = x + x * (x2 * (-1 / 6 + x2 * (1 / 120 + x2 * (-1 / 5040 + x2 * (1 / 362880)))))
    odd = turn % 2 == 1
    cos, sin = jnp.where(odd, sin, cos), jnp.where(odd, cos, sin)
    cos = jnp.where((turn == 1) | (turn == 2), -cos, cos)
    sin = jnp.where((turn == 2) | (turn == 3), -sin, sin)
    return cos, sin


def tables_kernel(place_ref, offsets_ref, taps_ref, weights_ref, interp_ref, base_ref, step_ref):
    tap_count = taps_ref.shape[1]
    chunk = 64
    wide = taps_ref.shape[2]

    @pl.loop(0, taps_ref.shape[0])
    def _(matrix):
        for lane in range(0, wide, LANES):
            cols = slice(lane, lane + LANES)
            for a in range(0, ANG, chunk):
                index = lax.broadcasted_iota(jnp.int32, (chunk, LANES), 0) + a
                summed = jnp.zeros((chunk, LANES), jnp.float32)
                for t in range(tap_count):
                    taps = taps_ref[matrix, t : t + 1, cols]
                    summed = summed + jnp.where(taps == index, weights_ref[matrix, t : t + 1, cols], 0.0)
                interp_ref[matrix, a : a + chunk, cols] = summed.astype(jnp.bfloat16)

    first_bin = place_ref[0]
    first_leaf = place_ref[1]
    for level in range(MERGES):

        @pl.loop(0, GROUP)
        def _(leaf):
            sector = jnp.int32(0)
            for j in range(level):
                sector = sector * 2 + (leaf >> j & 1)
            offset = offsets_ref[level, first_leaf + leaf]
            where = level * GROUP + leaf
            for lane in range(0, wide, LANES):
                cols = slice(lane, lane + LANES)
                angle = sector * wide + lane + lax.broadcasted_iota(jnp.int32, (8, LANES), 1)
                per_bin = offset * angle % phase_period
                bins = first_bin + GROUP * lax.broadcasted_iota(jnp.int32, (8, LANES), 0)
                cos, sin = unit_turn(per_bin * bins % phase_period)
                base_ref[where, 0, :, cols] = cos * inv_root_two
                base_ref[where, 1, :, cols] = sin * inv_root_two
                cos, sin = unit_turn(per_bin[:1] * (GROUP * 8) % phase_period)
                step_ref[where, 0:1, cols] = cos
                step_ref[where, 1:2, cols] = sin


def merge_tables(merge_taps, merge_weights, track_offsets, place):
    level_halves = 2 * MERGES
    taps = merge_taps.reshape(level_halves, *merge_taps.shape[2:])
    weights = merge_weights.reshape(level_halves, *merge_taps.shape[2:])
    wide = 2 * ANG
    return pl.pallas_call(
        tables_kernel,
        in_specs=[SMEM, SMEM, VMEM, VMEM],
        out_shape=(
            jax.ShapeDtypeStruct((level_halves, ANG, wide), jnp.bfloat16),
            jax.ShapeDtypeStruct((MERGES * GROUP, 2, 8, wide), jnp.float32),
            jax.ShapeDtypeStruct((MERGES * GROUP, 2, wide), jnp.float32),
        ),
        compiler_params=pltpu.CompilerParams(vmem_limit_bytes=VMEM_BYTES),
        name="merge_tables",
    )(place, track_offsets, taps, weights)


def product(a, b):
    return a[0] * b[0] - a[1] * b[1], a[0] * b[1] + a[1] * b[0]


def power(a, count):
    if count == 1:
        return a
    half = power(a, count // 2)
    whole = product(half, half)
    return product(whole, a) if count % 2 else whole


def merge_kernel(segments, pulses_hbm, beam_hbm, interp_hbm, base_hbm, step_hbm, out_hbm, *refs):
    pulses_ref, beam_ref, interp_ref, base_ref, step_ref, out_ref, image_ref, mixed_ref = refs[:8]
    pulse_sems, whole_sems, level_sems, out_sems = refs[8:]
    bins = pulses_ref.shape[2]
    parts = pulses_ref.shape[1]
    batch = 4

    def copy(source, target, here, sem):
        return pltpu.make_async_copy(source.at[here], target.at[here], sem)

    def pulses_copy(i):
        return copy(pulses_hbm, pulses_ref, pl.ds(i * batch, batch), pulse_sems.at[i])

    def level_copies(level):
        return (
            copy(interp_hbm, interp_ref, pl.ds(2 * level, 2), level_sems.at[level, 0]),
            copy(base_hbm, base_ref, pl.ds(level * GROUP, GROUP), level_sems.at[level, 1]),
        )

    def out_copy(leaf):
        return copy(out_ref, out_hbm, pl.ds(leaf, 1), out_sems.at[leaf])

    beam_copy = pltpu.make_async_copy(beam_hbm, beam_ref, whole_sems.at[0])
    step_copy = pltpu.make_async_copy(step_hbm, step_ref, whole_sems.at[1])
    beam_copy.start()
    for i in range(GROUP // batch):
        pulses_copy(i).start()
    step_copy.start()
    for level in range(MERGES):
        for item in level_copies(level):
            item.start()
    beam_copy.wait()

    @pl.loop(0, GROUP // batch)
    def _(step):
        pulses_copy(step).wait()
        leaves = pl.ds(step * batch, batch)
        held = jnp.concatenate(
            [pulses_ref[leaves, j].reshape(batch * bins, pulses_ref.shape[3]) for j in range(parts)], axis=1
        )
        formed = jnp.dot(held, beam_ref[...], preferred_element_type=jnp.float32).astype(jnp.bfloat16)
        for j in range(batch):
            rows = formed[j * bins : (j + 1) * bins]
            image_ref[step * batch + j, :bins] = rows[:, :ANG]
            image_ref[step * batch + j, bins:] = rows[:, ANG:]

    step_copy.wait()
    for level in range(MERGES):
        for item in level_copies(level):
            item.wait()

        def lower(index):
            return (index >> level << (level + 1)) | (index & ((1 << level) - 1))

        @pl.loop(0, GROUP // 2 // batch)
        def _(step):
            for side in range(2):
                leaves = [lower(step * batch + j) + (side << level) for j in range(batch)]
                held = jnp.concatenate([image_ref[leaf] for leaf in leaves])
                mixed = jnp.dot(held, interp_ref[2 * level + side], preferred_element_type=jnp.float32)
                for j in range(batch):
                    mixed_ref[side, step * batch + j] = mixed[j * 2 * bins : (j + 1) * 2 * bins]

        @pl.loop(0, GROUP // 2)
        def _(index):
            low = lower(index)
            pair = (low, low + (1 << level))
            for lane in range(0, 2 * ANG, 2 * LANES):
                cols = slice(lane, lane + 2 * LANES)
                turns, steps = [], []
                for side in range(2):
                    where = level * GROUP + pair[side]
                    base = tuple(base_ref[where, part, :, cols] for part in range(2))
                    step = tuple(step_ref[where, part : part + 1, cols] for part in range(2))
                    later = product(base, step)
                    turns.append(tuple(jnp.concatenate([base[part], later[part]]) for part in range(2)))
                    steps.append(product(step, step))
                target = pair[lane // ANG]
                place = 0
                spots = [start + i for start, count in segments for i in range(0, count, ROWS)]
                for row, spot in zip(range(0, bins, ROWS), spots):
                    if spot != place:
                        jumps = [power(steps[side], (spot - place) // ROWS) for side in range(2)]
                        turns = [product(turns[side], jumps[side]) for side in range(2)]
                        place = spot
                    real, imag = 0.0, 0.0
                    for side in range(2):
                        held = tuple(
                            mixed_ref[side, index, part * bins + row : part * bins + row + ROWS, cols]
                            for part in range(2)
                        )
                        r, i = product(turns[side], held)
                        real, imag = real + r, imag + i
                    if level == MERGES - 1:
                        out_ref[target, row : row + ROWS, :] = jnp.sqrt(real * real + imag * imag).astype(
                            out_ref.dtype
                        )
                    else:
                        image_ref[target, row : row + ROWS, :] = real.astype(jnp.bfloat16)
                        image_ref[target, bins + row : bins + row + ROWS, :] = imag.astype(jnp.bfloat16)
            if level == MERGES - 1:
                for leaf in pair:
                    out_copy(leaf).start()

    for leaf in range(GROUP):
        out_copy(leaf).wait()


def merged_magnitude(segments, pulses, beam, interp, base, step):
    bins = pulses.shape[2]
    inputs = (pulses, beam, interp, base, step)
    return pl.pallas_call(
        functools.partial(merge_kernel, segments),
        in_specs=[ANY] * len(inputs),
        out_specs=ANY,
        out_shape=jax.ShapeDtypeStruct((GROUP, bins, ANG), jnp.bfloat16),
        scratch_shapes=[
            *[pltpu.VMEM(array.shape, array.dtype) for array in inputs],
            pltpu.VMEM((GROUP, bins, ANG), jnp.bfloat16),
            pltpu.VMEM((GROUP, 2 * bins, ANG), jnp.bfloat16),
            pltpu.VMEM((2, GROUP // 2, 2 * bins, 2 * ANG), jnp.float32),
            pltpu.SemaphoreType.DMA((GROUP // 4,)),
            pltpu.SemaphoreType.DMA((2,)),
            pltpu.SemaphoreType.DMA((MERGES, 2)),
            pltpu.SemaphoreType.DMA((GROUP,)),
        ],
        compiler_params=pltpu.CompilerParams(vmem_limit_bytes=VMEM_BYTES),
        name="merged_magnitude",
    )(*inputs)


class Zone(typing.NamedTuple):
    pieces: tuple
    rows: int
    begin: int
    count: int
    place: int
    below: bool
    above: bool


def zones_of(chunks, bins):
    if len(chunks) == 1:
        return (Zone(((0, 0, bins, 8),), bins, 0, bins, 0, True, True),), ()
    (_, low), (high, top) = chunks[0]
    early = (
        Zone(((0, 0, low, 8),), low, 0, low - 8, 0, True, False),
        Zone(((0, low, top, 8),), top, 8, top - 8, high + 8, False, True),
    )
    middle = bins - low - top
    pieces = ((0, low - ROWS, ROWS, 0), (1, 0, middle, ROWS), (0, low, ROWS, ROWS + middle))
    late = (Zone(pieces, middle + 16, 0, middle + 16, low - 8, False, False),)
    return early, late


def diffuse_kernel(zones, array_count, *refs):
    cells_refs, out_hbm, scratch = refs[:array_count], refs[-1 - 4 * len(zones)], refs[-4 * len(zones) :]
    halo_refs = refs[array_count : array_count + 2] if any(zone.below or zone.above for zone in zones) else ()
    position = lax.axis_index("rng")
    first, last = position == 0, position == lax.axis_size("rng") - 1
    half = GROUP // 2
    blocks = [slice(h * LANES, (h + 1) * LANES) for h in range(ANG // LANES)]
    sublane = lax.broadcasted_iota(jnp.int32, (8, LANES), 0)
    if halo_refs:
        below_ref, above_ref = halo_refs
    held_zones = []
    for k, zone in enumerate(zones):
        held_zones.append((zone, *scratch[4 * k : 4 * k + 4]))

    def flux(upper, lower):
        difference = upper - lower
        return difference / (2.0 + difference * difference)

    sends = []
    for zone, out_ref, ping_ref, pong_ref, out_sems in held_zones:
        bins = zone.rows
        pitch = bins + 16
        for array, source, rows, start in zone.pieces:
            for h, cols in enumerate(blocks):
                for c in range(GROUP):
                    ping_ref[h, pl.ds(c * pitch + start, rows)] = (
                        cells_refs[array][c, source : source + rows, cols].astype(jnp.float32) * diffusion_scale
                    )
        for h, cols in enumerate(blocks):
            for j in range(half):
                if zone.below:
                    down = half + j
                    own = ping_ref[h, pl.ds((GROUP - 1 - down) * pitch + 8, 1)]
                    sent = below_ref[j : j + 1, cols].astype(jnp.float32) * diffusion_scale
                    ping_ref[h, pl.ds(down * pitch + 7, 1)] = jnp.where(first, own, sent)
                if zone.above:
                    own = ping_ref[h, pl.ds((GROUP - 1 - j) * pitch + 7 + bins, 1)]
                    sent = above_ref[j : j + 1, cols].astype(jnp.float32) * diffusion_scale
                    ping_ref[h, pl.ds(j * pitch + 8 + bins, 1)] = jnp.where(last, own, sent)

        def tile(source, target, h, row, begin, end):
            def cells(c, shift=0):
                return source[h, pl.ds(c * pitch + row + shift, 8)]

            def before():
                near, far = pltpu.roll(cells(GROUP - 1), 1, 0), pltpu.roll(cells(GROUP - 1, -8), 1, 0)
                return jnp.where(sublane == 0, far, near)

            def after():
                near, far = pltpu.roll(cells(0), 7, 0), pltpu.roll(cells(0, 8), 7, 0)
                return jnp.where(sublane == 7, far, near)

            here = cells(begin)
            flow = flux(here, before()) if begin == 0 else None
            for c in range(begin, end):
                if c < end - 1:
                    there = cells(c + 1)
                elif end == GROUP:
                    there = after()
                else:
                    there = None
                ahead = flux(there, here) if there is not None else None
                value = here
                if ahead is not None:
                    value = value + ahead
                if flow is not None:
                    value = value - flow
                target[h, pl.ds(c * pitch + row, 8)] = value
                here, flow = there, ahead

        def sweep(source, target):
            for h in range(len(blocks)):
                if zone.below or zone.begin == 0:
                    tile(source, target, h, 0, half, GROUP)
                if zone.above or zone.begin + zone.count == bins:
                    tile(source, target, h, 8 + bins, 0, half)

            @pl.loop(0, bins // 8)
            def _(step):
                for h in range(len(blocks)):
                    tile(source, target, h, pl.multiple_of(8 + 8 * step, 8), 0, GROUP)

        @pl.loop(0, SWEEPS // 2)
        def _(step):
            sweep(ping_ref, pong_ref)
            sweep(pong_ref, ping_ref)

        rows = LANES // GROUP

        def out_copy(step, zone=zone, out_ref=out_ref, out_sems=out_sems):
            here = pl.ds(pl.multiple_of(step * LANES, LANES), LANES)
            there = pl.ds(pl.multiple_of(zone.place * GROUP + step * LANES, LANES), LANES)
            return pltpu.make_async_copy(out_ref.at[:, here], out_hbm.at[:, there], out_sems.at[step])

        @pl.loop(0, zone.count // rows)
        def _(step):
            for h, cols in enumerate(blocks):
                held = jnp.concatenate(
                    [
                        ping_ref[h, pl.ds(8 + zone.begin + step * rows + d, GROUP, stride=pitch)]
                        for d in range(rows)
                    ]
                )
                here = pl.ds(pl.multiple_of(step * LANES, LANES), LANES)
                out_ref[cols, here] = held.T * (1.0 / diffusion_scale)
            out_copy(step).start()

        sends.append((out_copy, zone.count // rows))

    for out_copy, count in sends:
        for step in range(count):
            out_copy(step).wait()


def despeckle(zones, cells, halo, bins, started=()):
    shape = (ANG, GROUP * bins)
    scratch = []
    for zone in zones:
        held = pltpu.VMEM((ANG // LANES, GROUP * (zone.rows + 16), LANES), jnp.float32)
        scratch += [
            pltpu.VMEM((ANG, GROUP * zone.count), jnp.float32),
            held,
            held,
            pltpu.SemaphoreType.DMA((GROUP * zone.count // LANES,)),
        ]
    return pl.pallas_call(
        functools.partial(diffuse_kernel, zones, len(cells)),
        in_specs=[VMEM] * (len(cells) + len(halo)) + [ANY] * len(started),
        out_specs=ANY,
        out_shape=jax.ShapeDtypeStruct(shape, jnp.float32),
        scratch_shapes=scratch,
        input_output_aliases={len(cells): 0} if started else {},
        compiler_params=pltpu.CompilerParams(vmem_limit_bytes=14 << 20),
        name="despeckle",
    )(*cells, *halo, *started)


def per_device(raw_echoes, merge_taps, merge_weights, track_offsets):
    sub_count, rng_count = lax.axis_size("sub"), lax.axis_size("rng")
    leaf, position = lax.axis_index("sub"), lax.axis_index("rng")
    pulses, samples = raw_echoes.shape[1:]
    bins = samples // (GROUP * rng_count)
    groups = [[g * GROUP + i for i in range(GROUP)] for g in range(sub_count // GROUP)]
    groups = groups if len(groups) > 1 else None

    chunks = chunked(bins)

    def regroup(block, count):
        if groups is None:
            block = block.reshape(GROUP * rng_count, 2 * count, pulses)
            block = lax.all_to_all(block, ("sub", "rng"), split_axis=0, concat_axis=0, tiled=True)
        else:
            block = block.reshape(GROUP, rng_count, 2 * count, pulses)
            block = lax.all_to_all(block, "rng", split_axis=1, concat_axis=1, tiled=True)
            block = lax.all_to_all(
                block, "sub", split_axis=0, concat_axis=0, tiled=True, axis_index_groups=groups
            )
        return block.reshape(GROUP, rng_count * 2, count, pulses)

    compressed = []
    for segments in chunks:
        if compressed:
            raw_echoes, compressed[-1] = lax.optimization_barrier((raw_echoes, compressed[-1]))
        compressed.append(range_transform(segments, raw_echoes, rng_count))
    place = jnp.stack([leaf % GROUP + 1 + position * (bins * GROUP), leaf // GROUP * GROUP]).astype(jnp.int32)
    tables = merge_tables(merge_taps, merge_weights, track_offsets, place)
    regrouped = []
    for block, segments in zip(compressed, chunks):
        if regrouped:
            block, tables, regrouped[-1] = lax.optimization_barrier((block, tables, regrouped[-1]))
        regrouped.append(regroup(block, length(segments)))
    beam = jnp.asarray(beam_table(pulses * rng_count, rng_count))
    cells = []
    for segments, block in zip(chunks, regrouped):
        magnitude = merged_magnitude(segments, block, beam, *tables)
        cells.append(
            lax.all_to_all(magnitude, "sub", split_axis=0, concat_axis=0, tiled=True, axis_index_groups=groups)
        )
    half = GROUP // 2
    head, tail = cells[0][:half, 0], cells[0][half:, -1]
    if rng_count == 2:
        below = above = lax.ppermute(jnp.where(position == 0, tail, head), "rng", [(0, 1), (1, 0)])
    else:
        ends = rng_count - 1
        below = lax.ppermute(tail, "rng", [(i, i + 1) for i in range(ends)])
        above = lax.ppermute(head, "rng", [(i + 1, i) for i in range(ends)])
    early, late = zones_of(chunks, bins)
    result = despeckle(early, cells[:1], (below, above), bins)
    if late:
        result = despeckle(late, cells, (), bins, (result,))
    return result


def solution(mesh):
    in_specs = (P(None, ("sub", "rng"), None), P(), P(), P())
    out_specs = P("sub", "rng")
    return jax.shard_map(
        per_device, mesh=mesh, in_specs=in_specs, out_specs=out_specs, check_vma=False
    )
```
